32 devices in a mesh: groups: 2 (over y), batch: 8 (over z, x), heads: 2 (over core).
Axes of the slice: x: 2, y: 2, z: 4, core: 2. Of those that a mesh axis runs over, the one named last changes fastest.
Arguments:
- storage: bfloat16 [1, 4096, 4608], P(None, ('groups', 'batch', 'heads')), parts along dimension 1, may hold values from -6 to 6
- block_table: int32 [4096], P('groups'), parts along dimension 0, may hold values from 0 to 2047, as said below
- lengths: int32 [16], P(('groups', 'batch')), parts along dimension 0, may hold values from 4 to 2048
- query: bfloat16 [16, 4, 128, 576], P(('groups', 'batch'), None, 'heads'), parts along dimension 0, may hold values from -10 to 10
Outputs:
- context: bfloat16 [16, 4, 128, 512], P(('groups', 'batch'), None, 'heads'), parts along dimension 0
The draws below stay inside these ranges and needn't reach their ends.
There are 2 independent parts, one for each index of `groups`. The reference program is written for one: setup_inputs(seed, part) draws one part's arguments, and reference() takes and returns one part's arrays. A program takes and returns all parts, laid end to end along the dimension named above; each array names one. Nothing has to cross between parts.
Inputs may be any that keep to these rules, and one draw needn't show every extreme that they name: `block_table`: the entries are a permutation of 0 to 2047; entry g names block g mod 256 of sequence g // 256. Storage device k of the batch+heads order, with k = 2 b + p, holds for every batch index j exactly 16 blocks of sequences j * 1 to (j + 1) - 1, all with block numbers from p * 128 to (p + 1) * 128 - 1, in no particular order.
All inputs are finite; a program needn't handle non-finite values.
Results may differ from the reference program's by a relative error of at most 0.0031.
Values may be sent and summed in bfloat16 or wider, within the bound.
A program may use at most 64 MiB of HBM per device.

```python
import math
import jax
import jax.numpy as jnp
from jax import lax

LATENT = 512
ROPE = 64
QHEADS = 128
HEAD_NOPE = 128
SEQ_DEV = 1
MAXLEN = 2048
BLK = 8
QTOK = 4
LAYERS = 1
KVW = 576
NBLK = 256
HALF = 128
SEQS = 8
SLOTS = 2048
SLOT_DEV = 128
BLK_PEER = 16
N_BATCH = 8
N_HEADS = 2


def draw_storage(key, part):
    shape = (LAYERS, SLOTS, BLK * KVW)
    values = jnp.clip(jax.random.normal(jax.random.fold_in(key, 3), shape, jnp.float32), -4.0, 4.0)
    return values.astype(jnp.bfloat16)


def draw_query(key, part):
    shape = (SEQS, QTOK, QHEADS, KVW)
    values = jnp.clip(jax.random.normal(jax.random.fold_in(key, 5), shape, jnp.float32), -4.0, 4.0)
    return values.astype(jnp.bfloat16)


def draw_block_table(key, part):
    item_count = SEQ_DEV * HALF
    deal_keys = jax.random.split(jax.random.fold_in(key, 11), N_HEADS * N_BATCH)
    dealt = jax.vmap(lambda single: jax.random.permutation(single, item_count))(deal_keys)
    dealt = dealt.reshape(N_HEADS, N_BATCH, item_count).astype(jnp.int32)
    half_index = jnp.arange(N_HEADS, dtype=jnp.int32)[:, None, None]
    owner_index = jnp.arange(N_BATCH, dtype=jnp.int32)[None, :, None]
    sequence = owner_index * SEQ_DEV + dealt // HALF
    block = half_index * HALF + dealt % HALF
    labels = (sequence * NBLK + block).reshape(N_HEADS, N_BATCH, N_BATCH, BLK_PEER)
    labels = jnp.transpose(labels, (2, 0, 1, 3)).reshape(N_BATCH * N_HEADS, SLOT_DEV)
    shuffle_keys = jax.random.split(jax.random.fold_in(key, 13), N_BATCH * N_HEADS)
    shuffles = jax.vmap(lambda single: jax.random.permutation(single, SLOT_DEV))(shuffle_keys).astype(jnp.int32)
    labels = jnp.take_along_axis(labels, shuffles, axis=1)
    return labels.reshape(SLOTS).astype(jnp.int32)


def set_ends(entries, rng, smallest, high):
    longest = entries.shape.index(max(entries.shape))
    spots = []
    for shift in (0, 1):
        where = [jax.random.randint(jax.random.fold_in(rng, axis), (), 0, length) for axis, length in enumerate(entries.shape)]
        where[longest] = (where[longest] + shift) % entries.shape[longest]
        spots.append(tuple(where))
    return entries.at[spots[0]].set(smallest).at[spots[1]].set(high)


def setup_inputs(seed: int = 0, part: int = 0) -> dict:
    seeds = jax.random.split(jax.random.key(seed), 5)
    part_splits = jax.random.split(jax.random.fold_in(seeds[4], part), 5)
    storage = draw_storage(jax.random.fold_in(jax.random.fold_in(seeds[4], part), 71), part)
    block_table = draw_block_table(jax.random.fold_in(jax.random.fold_in(seeds[4], part), 71), part)
    lengths = set_ends(jax.random.randint(part_splits[2], (SEQS,), QTOK, MAXLEN + 1), jax.random.fold_in(part_splits[2], 1), QTOK, MAXLEN).astype(jnp.int32)
    query = draw_query(jax.random.fold_in(jax.random.fold_in(seeds[4], part), 71), part)
    return {"storage": storage, "block_table": block_table, "lengths": lengths, "query": query}


def reference(storage, block_table, lengths, query):
    slot_total = block_table.shape[0]
    inverse = jnp.zeros((slot_total,), jnp.int32).at[block_table].set(jnp.arange(slot_total, dtype=jnp.int32))
    cache = jnp.take(storage[0], inverse, axis=0).reshape(SEQS, MAXLEN, KVW)
    score_scale = 1.0 / math.sqrt(HEAD_NOPE + ROPE)
    draft = jnp.arange(QTOK * QHEADS, dtype=jnp.int32) // QHEADS
    places = jnp.arange(MAXLEN, dtype=jnp.int32)

    def one_sequence(packed):
        key_rows, query_rows, length = packed
        flat = query_rows.reshape(QTOK * QHEADS, KVW)
        scores = jnp.dot(flat, key_rows.T, preferred_element_type=jnp.float32) * score_scale
        limit = length - QTOK + draft
        visible = places[None, :] <= limit[:, None]
        masked = jnp.where(visible, scores, -1e+30)
        peak = lax.optimization_barrier(jnp.max(masked, axis=1, keepdims=True))
        raised = jnp.where(visible, jnp.exp(masked - peak), 0.0)
        totals = lax.optimization_barrier(jnp.sum(raised, axis=1, keepdims=True))
        mixed = jnp.dot(raised.astype(jnp.bfloat16), key_rows[:, :LATENT], preferred_element_type=jnp.float32)
        return (mixed / totals).astype(jnp.bfloat16).reshape(QTOK, QHEADS, LATENT)
    return lax.map(one_sequence, (cache, query, lengths))
```

```python
import functools
import math

import jax
import jax.numpy as jnp
from jax import lax
from jax.experimental import pallas as pl
from jax.experimental.pallas import tpu as pltpu
from jax.sharding import PartitionSpec as P

MESH = pl.DeviceIdType.MESH
NT = (((1,), (1,)), ((), ()))
LATENT = 512
ROPE = 64
HEAD_NOPE = 128
SEQ_DEV = 1
MAXLEN = 2048
BLK = 8
QTOK = 4
AHEAD = 1


def partial_softmax(query_rows, key_rows, first_place, limits, score_scale):
    scores = (
        jnp.einsum("src,stc->srt", query_rows, key_rows, preferred_element_type=jnp.float32)
        * score_scale
    )
    places = first_place + jnp.arange(key_rows.shape[1], dtype=jnp.int32)
    visible = places[None, None, :] <= limits[:, :, None]
    masked = jnp.where(visible, scores, -1e30)
    highest = jnp.max(masked, axis=2)
    raised = jnp.where(visible, jnp.exp(masked - highest[:, :, None]), 0.0)
    totals = jnp.sum(raised, axis=2)
    mixed = jnp.einsum(
        "srt,stc->src",
        raised.astype(jnp.bfloat16),
        key_rows[:, :, :LATENT],
        preferred_element_type=jnp.float32,
    )
    return (highest, totals, mixed)


def plain_local(storage, block_table, lengths, query):
    batch_count = lax.axis_size("batch")
    head_groups = lax.axis_size("heads")
    my_batch = lax.axis_index("batch")
    my_half = lax.axis_index("heads")
    slot_count = storage.shape[1]
    per_peer = slot_count // batch_count
    block_count = MAXLEN // BLK
    half_blocks = block_count // head_groups
    width = LATENT + ROPE
    zero_index = jnp.zeros((), jnp.int32)
    table_grid = block_table.reshape(batch_count, head_groups, slot_count)
    own_table = lax.dynamic_slice(
        table_grid, (my_batch, my_half, zero_index), (1, 1, slot_count)
    ).reshape(slot_count)
    owner = own_table // block_count // SEQ_DEV
    owner_table = (owner[:, None] == jnp.arange(batch_count, dtype=jnp.int32)[None, :]).astype(
        jnp.int32
    )
    rank = jnp.sum(owner_table * (jnp.cumsum(owner_table, axis=0) - 1), axis=1)
    send_place = owner * per_peer + rank
    order = (
        jnp.zeros((slot_count,), jnp.int32)
        .at[send_place]
        .set(jnp.arange(slot_count, dtype=jnp.int32))
    )
    outgoing = jnp.take(storage, order, axis=1)
    received = lax.all_to_all(outgoing, "batch", split_axis=1, concat_axis=1, tiled=True)
    sender_table = lax.dynamic_slice(
        table_grid, (zero_index, my_half, zero_index), (batch_count, 1, slot_count)
    ).reshape(batch_count, slot_count)
    sequence_ids = sender_table // block_count
    arrivals = sequence_ids // SEQ_DEV == my_batch
    arrive_place = (
        jnp.arange(batch_count, dtype=jnp.int32)[:, None] * per_peer
        + jnp.cumsum(arrivals.astype(jnp.int32), axis=1)
        - 1
    )
    target = (
        (sequence_ids - my_batch * SEQ_DEV) * half_blocks
        + sender_table % block_count
        - my_half * half_blocks
    )
    target = jnp.where(arrivals, target, slot_count)
    source = (
        jnp.zeros((slot_count,), jnp.int32)
        .at[target.reshape(-1)]
        .set(arrive_place.reshape(-1), mode="drop")
    )
    serving = jnp.take(received, source, axis=1)
    half_length = half_blocks * BLK
    seq_count = query.shape[0]
    local_keys = serving[0].reshape(seq_count, half_length * width)
    score_scale = 1.0 / math.sqrt(HEAD_NOPE + ROPE)
    every_query = lax.all_gather(query, "heads", axis=2, tiled=True)
    all_heads = every_query.shape[2]
    row_count = QTOK * all_heads
    query_rows = every_query.reshape(seq_count, row_count, width)
    draft = jnp.arange(row_count, dtype=jnp.int32) // all_heads
    limits = lengths[:, None] - QTOK + draft[None, :]
    key_rows = local_keys.reshape(seq_count, half_length, width)
    highest, totals, mixed = partial_softmax(
        query_rows, key_rows, my_half * half_length, limits, score_scale
    )
    shaped = (
        highest.reshape(1, seq_count, QTOK, all_heads),
        totals.reshape(1, seq_count, QTOK, all_heads),
        mixed.reshape(1, seq_count, QTOK, all_heads, LATENT),
    )
    pieces = (
        lax.all_to_all(shaped[0], "heads", split_axis=3, concat_axis=0, tiled=True),
        lax.all_to_all(shaped[1], "heads", split_axis=3, concat_axis=0, tiled=True),
        lax.all_to_all(shaped[2], "heads", split_axis=3, concat_axis=0, tiled=True),
    )
    overall = jnp.max(pieces[0], axis=0)
    factor = jnp.exp(pieces[0] - overall[None])
    totals = jnp.sum(pieces[1] * factor, axis=0)
    mixed = jnp.sum(pieces[2] * factor[..., None], axis=0)
    context = (mixed / totals[..., None]).astype(jnp.bfloat16)
    return context


def send_orders(batch_count):
    whole = list(range(1, batch_count))
    if batch_count != 8:
        return [whole] * 4, [[0] + whole] * 4
    sends = [
        [1, 2, 3, 4, 5, 6, 7],
        [6, 7, 4, 5, 2, 3, 1],
        [6, 4, 5, 7, 2, 3, 1],
        [6, 7, 2, 3, 4, 5, 1],
    ]
    uses = [
        [0, 1, 2, 3, 4, 6, 5, 7],
        [0, 1, 6, 2, 3, 7, 4, 5],
        [0, 1, 6, 7, 4, 2, 5, 3],
        [0, 1, 2, 3, 4, 5, 6, 7],
    ]
    return sends, uses


def fused_kernel(
    batch_count, table_ref, length_ref, storage_ref, query_ref, out_ref,
    tabled, lengthy, stored, asked, outgoing, keys, queries, places, mixed,
    load_sem, fetch_sem, send_sem, recv_sem, pass_sem, take_sem, ready_sem,
):
    slot_count = stored.shape[0]
    per_peer = slot_count // batch_count
    block_count = MAXLEN // BLK
    width = LATENT + ROPE
    span = 2 * width
    pieces = BLK // 2
    me = lax.axis_index("batch")
    half = lax.axis_index("heads")
    sibling = 1 - half
    depth = me // 2
    deep = batch_count // 2
    left = depth == deep // 2 - 1
    right = depth == deep // 2
    middle = left | right
    across = batch_count - 2
    sends, uses = send_orders(batch_count)
    kind = jnp.where(left, 1, jnp.where(right, 2, jnp.where(depth < deep // 2, 0, 3)))

    def flip(step):
        other = me
        bit = 1
        while bit < batch_count:
            other = other + bit * (1 - 2 * ((me // bit) % 2)) * ((step // bit) % 2)
            bit *= 2
        return other

    def chosen(table, place):
        picked = table[3][place]
        for index in range(3):
            picked = jnp.where(kind == index, table[index][place], picked)
        return picked

    def columns(piece):
        return pl.ds(piece * span, span)

    def rows(index):
        return pl.ds(pl.multiple_of(index * per_peer, per_peer), per_peer)

    load_table = pltpu.make_async_copy(table_ref, tabled, load_sem.at[0])
    load_query = pltpu.make_async_copy(query_ref, asked, load_sem.at[1])
    load_length = pltpu.make_async_copy(length_ref, lengthy, load_sem.at[2])
    fetches = [
        pltpu.make_async_copy(
            storage_ref.at[:, columns(piece)], stored.at[:, columns(piece)], fetch_sem.at[piece]
        )
        for piece in range(pieces)
    ]
    load_table.start()
    for fetch in fetches:
        fetch.start()

    barrier = pltpu.get_barrier_semaphore()

    def tell(other, core):
        pl.semaphore_signal(
            barrier, inc=1, device_id={"batch": other, "heads": core}, device_id_type=MESH
        )

    @pl.when(middle)
    def _():
        tell(flip(across), half)

    for spot in range(batch_count):
        if spot // 2 in (deep // 2 - 1, deep // 2):
            continue
        for core in range(2):

            @pl.when((me != spot) | (half != core))
            def _():
                tell(spot, core)

    load_query.start()
    load_length.start()

    load_table.wait()
    table = tabled[...]
    row_ids = lax.broadcasted_iota(jnp.int32, table.shape, 0)
    square = (slot_count, slot_count)
    down = lax.broadcasted_iota(jnp.int32, square, 0)
    along = lax.broadcasted_iota(jnp.int32, square, 1)
    earlier = (down < along).astype(jnp.float32).astype(jnp.bfloat16)
    own = jnp.sum(jnp.where(row_ids == 2 * me + half, table, 0), axis=0, keepdims=True)
    owner = own // block_count
    belongs = (row_ids == owner).astype(jnp.float32)
    counts = jnp.dot(belongs.astype(jnp.bfloat16), earlier, preferred_element_type=jnp.float32)
    rank = jnp.sum(belongs * counts, axis=0, keepdims=True).astype(jnp.int32)
    place = owner * per_peer + rank
    order = (down == place).astype(jnp.float32).astype(jnp.bfloat16)

    lanes = lax.broadcasted_iota(jnp.int32, (1, 2 * ROPE), 1)
    first_lanes = (lanes < ROPE).astype(jnp.float32).astype(jnp.bfloat16)
    last_lanes = (lanes >= ROPE).astype(jnp.float32).astype(jnp.bfloat16)

    def group(piece):
        fetches[piece].wait()
        base = piece * span
        moved = jnp.dot(
            order, stored[:, columns(piece)], preferred_element_type=jnp.float32
        )
        outgoing[:, base : base + LATENT] = moved[:, :LATENT].astype(jnp.bfloat16)
        outgoing[:, base + LATENT : base + 2 * LATENT] = moved[
            :, width : width + LATENT
        ].astype(jnp.bfloat16)
        outgoing[:, base + 2 * LATENT : base + span] = jnp.where(
            lanes < ROPE, moved[:, LATENT : LATENT + 2 * ROPE], moved[:, span - 2 * ROPE :]
        ).astype(jnp.bfloat16)

    def send(step, where):
        other = flip(step)
        return pltpu.make_async_remote_copy(
            src_ref=outgoing.at[rows(other), where],
            dst_ref=keys.at[half, rows(me), where],
            send_sem=send_sem.at[step],
            recv_sem=recv_sem.at[step],
            device_id={"batch": other},
            device_id_type=MESH,
        )

    everything = pl.ds(0, pieces * span)

    def arrival(step):
        other = flip(step)
        return pltpu.make_async_remote_copy(
            src_ref=outgoing.at[rows(other), everything],
            dst_ref=keys.at[half, rows(other), everything],
            send_sem=send_sem.at[step],
            recv_sem=recv_sem.at[step],
            device_id={"batch": other},
            device_id_type=MESH,
        )

    def hand_over(step, source):
        other = flip(step)
        return pltpu.make_async_remote_copy(
            src_ref=source.at[rows(other)],
            dst_ref=keys.at[half, rows(other)],
            send_sem=pass_sem.at[step],
            recv_sem=take_sem.at[step],
            device_id={"heads": sibling},
            device_id_type=MESH,
        )

    for piece in range(pieces):
        group(piece)

        @pl.when(middle)
        def _():
            if piece == 0:
                pl.semaphore_wait(barrier, 1)
            send(across, columns(piece)).start()

    @pl.when(middle)
    def _():
        pl.semaphore_wait(ready_sem, 1)

    @pl.when(jnp.logical_not(middle))
    def _():
        pl.semaphore_wait(barrier, 2 * batch_count - 1)

        @pl.when((depth == 0) | (depth == deep - 1))
        def _():
            inner = jnp.where(depth == 0, me + batch_count - 2 - deep, me - batch_count + 2 + deep)
            pl.semaphore_signal(
                ready_sem, inc=1, device_id={"batch": inner}, device_id_type=MESH
            )

        send(chosen(sends, 0), everything).start()

    for turn in range(1, batch_count - 1):
        send(chosen(sends, turn), everything).start()
    hand_over(0, outgoing).start()

    keys[half, rows(me)] = outgoing[rows(me)]

    mine = table // block_count == me
    marks = mine.astype(jnp.float32)
    ranks = jnp.dot(
        marks.astype(jnp.bfloat16), earlier, preferred_element_type=jnp.float32
    ).astype(jnp.int32)
    ranks = jnp.where(mine, ranks, -1)
    blocks = (table % block_count).astype(jnp.float32)
    lane = lax.broadcasted_iota(jnp.int32, table.shape, 1)
    spots = (lane // per_peer).astype(jnp.float32)
    for index in range(per_peer):
        number = jnp.sum(jnp.where(ranks == index, blocks, 0.0), axis=1, keepdims=True)
        spots = spots + jnp.where(lane % per_peer == index, number * BLK, 0.0)
    places[...] = spots

    row_count = asked.shape[0]
    heads = row_count // QTOK
    load_length.wait()
    limits = [(lengthy[0] - QTOK + draft).astype(jnp.float32) for draft in range(QTOK)]

    load_query.wait()
    asking = asked[...]
    queries[:, :width] = asking
    queries[:, width:] = asking[:, LATENT:]

    factor = math.log2(math.e) / math.sqrt(HEAD_NOPE + ROPE)
    peak = jnp.full((row_count, 1), -1e30, jnp.float32)
    totals = jnp.zeros((row_count, slot_count), jnp.float32)
    steps = [0] + [chosen(uses, turn) for turn in range(1, batch_count)]
    for turn in range(batch_count):
        if turn + AHEAD < batch_count:
            for ahead in range(1 if turn == 0 else turn + AHEAD, turn + AHEAD + 1):
                arrival(steps[ahead]).wait_recv()
                hand_over(steps[ahead], keys.at[half]).start()
        step = steps[turn]
        other = me if turn == 0 else flip(step)
        hand_over(step, keys.at[half]).wait_recv()
        latents = []
        ropes = []
        for core in range(2):
            for piece in range(pieces):
                base = piece * span
                pair = keys[core, rows(other), base + 2 * LATENT : base + span]
                for parity in range(2):
                    low = base + parity * LATENT
                    latents.append(keys[core, rows(other), low : low + LATENT])
                    ropes.append(pair * (last_lanes if parity else first_lanes))
        latent = jnp.concatenate(latents, axis=0)
        rope = jnp.concatenate(ropes, axis=0)
        dots = lax.dot_general(
            queries[...],
            jnp.concatenate([latent, rope], axis=1),
            NT,
            preferred_element_type=jnp.float32,
        )
        at = places[pl.ds(2 * other, 2), :]
        at = jnp.concatenate([at[0:1], at[1:2]], axis=1)
        scores = jnp.concatenate(
            [
                dots[draft * heads : (draft + 1) * heads]
                + jnp.where(at <= limits[draft], 0.0, -1e30)
                for draft in range(QTOK)
            ],
            axis=0,
        )
        higher = jnp.maximum(peak, jnp.max(scores, axis=1, keepdims=True))
        raised = jnp.exp2((scores - higher) * factor)
        sums = raised[:, :slot_count] + raised[:, slot_count:]
        fresh = jnp.dot(raised.astype(jnp.bfloat16), latent, preferred_element_type=jnp.float32)
        if turn == 0:
            totals = sums
            mixed[...] = fresh
        else:
            shrink = jnp.exp2((peak - higher) * factor)
            totals = totals * shrink + sums
            mixed[...] = mixed[...] * shrink + fresh
        peak = higher
    total = jnp.sum(totals, axis=1, keepdims=True)
    out_ref[...] = (mixed[...] / total).astype(out_ref.dtype)
    for step in range(1, batch_count):
        send(step, everything).wait_send()
    for step in range(batch_count):
        hand_over(step, keys.at[half]).wait_send()


def local(storage, block_table, lengths, query):
    batch_count = lax.axis_size("batch")
    slot_count = storage.shape[1]
    per_peer = slot_count // batch_count
    whole = batch_count & (batch_count - 1) == 0 and query.shape[0] == SEQ_DEV
    whole = whole and batch_count >= 8 and lax.axis_size("heads") == 2
    if per_peer % 16 or slot_count != 128 or BLK * per_peer != slot_count or not whole:
        return plain_local(storage, block_table, lengths, query)
    width = LATENT + ROPE
    heads = query.shape[2]
    row_count = QTOK * heads
    vmem = pl.BlockSpec(memory_space=pltpu.VMEM)
    anywhere = pl.BlockSpec(memory_space=pltpu.HBM)
    context = pl.pallas_call(
        functools.partial(fused_kernel, batch_count),
        out_shape=jax.ShapeDtypeStruct((row_count, LATENT), jnp.bfloat16),
        in_specs=[anywhere] * 4,
        out_specs=vmem,
        scratch_shapes=[
            pltpu.VMEM((block_table.shape[0] // slot_count, slot_count), jnp.int32),
            pltpu.SMEM(lengths.shape, jnp.int32),
            pltpu.VMEM((slot_count, BLK * width), jnp.bfloat16),
            pltpu.VMEM((row_count, width), jnp.bfloat16),
            pltpu.VMEM((slot_count, BLK * width), jnp.bfloat16),
            pltpu.VMEM((2, slot_count, BLK * width), jnp.bfloat16),
            pltpu.VMEM((row_count, LATENT + 2 * ROPE), jnp.bfloat16),
            pltpu.VMEM((block_table.shape[0] // slot_count, slot_count), jnp.float32),
            pltpu.VMEM((row_count, LATENT), jnp.float32),
            pltpu.SemaphoreType.DMA((3,)),
            pltpu.SemaphoreType.DMA((BLK // 2,)),
            pltpu.SemaphoreType.DMA((batch_count,)),
            pltpu.SemaphoreType.DMA((batch_count,)),
            pltpu.SemaphoreType.DMA((batch_count,)),
            pltpu.SemaphoreType.DMA((batch_count,)),
            pltpu.SemaphoreType.REGULAR,
        ],
        compiler_params=pltpu.CompilerParams(collective_id=0, has_side_effects=True, vmem_limit_bytes=54800 * 1024),
    )(
        block_table.reshape(-1, slot_count),
        lengths,
        storage[0],
        query.reshape(row_count, width),
    )
    return context.reshape(1, QTOK, heads, LATENT)


def solution(mesh):
    in_specs = (
        P(None, ("groups", "batch", "heads"), None),
        P("groups"),
        P(("groups", "batch")),
        P(("groups", "batch"), None, "heads", None),
    )
    out_specs = P(("groups", "batch"), None, "heads", None)
    return jax.shard_map(local, mesh=mesh, in_specs=in_specs, out_specs=out_specs, check_vma=False)
```

```python
import functools
import math

import jax
import jax.numpy as jnp
from jax import lax
from jax.experimental import pallas as pl
from jax.experimental.pallas import tpu as pltpu
from jax.sharding import PartitionSpec as P

MESH = pl.DeviceIdType.MESH
NT = (((1,), (1,)), ((), ()))
LATENT = 512
ROPE = 64
HEAD_NOPE = 128
SEQ_DEV = 1
MAXLEN = 2048
BLK = 8
QTOK = 4
AHEAD = 2


def partial_softmax(query_rows, key_rows, first_place, limits, score_scale):
    scores = (
        jnp.einsum("src,stc->srt", query_rows, key_rows, preferred_element_type=jnp.float32)
        * score_scale
    )
    places = first_place + jnp.arange(key_rows.shape[1], dtype=jnp.int32)
    visible = places[None, None, :] <= limits[:, :, None]
    masked = jnp.where(visible, scores, -1e30)
    highest = jnp.max(masked, axis=2)
    raised = jnp.where(visible, jnp.exp(masked - highest[:, :, None]), 0.0)
    totals = jnp.sum(raised, axis=2)
    mixed = jnp.einsum(
        "srt,stc->src",
        raised.astype(jnp.bfloat16),
        key_rows[:, :, :LATENT],
        preferred_element_type=jnp.float32,
    )
    return (highest, totals, mixed)


def plain_local(storage, block_table, lengths, query):
    batch_count = lax.axis_size("batch")
    head_groups = lax.axis_size("heads")
    my_batch = lax.axis_index("batch")
    my_half = lax.axis_index("heads")
    slot_count = storage.shape[1]
    per_peer = slot_count // batch_count
    block_count = MAXLEN // BLK
    half_blocks = block_count // head_groups
    width = LATENT + ROPE
    zero_index = jnp.zeros((), jnp.int32)
    table_grid = block_table.reshape(batch_count, head_groups, slot_count)
    own_table = lax.dynamic_slice(
        table_grid, (my_batch, my_half, zero_index), (1, 1, slot_count)
    ).reshape(slot_count)
    owner = own_table // block_count // SEQ_DEV
    owner_table = (owner[:, None] == jnp.arange(batch_count, dtype=jnp.int32)[None, :]).astype(
        jnp.int32
    )
    rank = jnp.sum(owner_table * (jnp.cumsum(owner_table, axis=0) - 1), axis=1)
    send_place = owner * per_peer + rank
    order = (
        jnp.zeros((slot_count,), jnp.int32)
        .at[send_place]
        .set(jnp.arange(slot_count, dtype=jnp.int32))
    )
    outgoing = jnp.take(storage, order, axis=1)
    received = lax.all_to_all(outgoing, "batch", split_axis=1, concat_axis=1, tiled=True)
    sender_table = lax.dynamic_slice(
        table_grid, (zero_index, my_half, zero_index), (batch_count, 1, slot_count)
    ).reshape(batch_count, slot_count)
    sequence_ids = sender_table // block_count
    arrivals = sequence_ids // SEQ_DEV == my_batch
    arrive_place = (
        jnp.arange(batch_count, dtype=jnp.int32)[:, None] * per_peer
        + jnp.cumsum(arrivals.astype(jnp.int32), axis=1)
        - 1
    )
    target = (
        (sequence_ids - my_batch * SEQ_DEV) * half_blocks
        + sender_table % block_count
        - my_half * half_blocks
    )
    target = jnp.where(arrivals, target, slot_count)
    source = (
        jnp.zeros((slot_count,), jnp.int32)
        .at[target.reshape(-1)]
        .set(arrive_place.reshape(-1), mode="drop")
    )
    serving = jnp.take(received, source, axis=1)
    half_length = half_blocks * BLK
    seq_count = query.shape[0]
    local_keys = serving[0].reshape(seq_count, half_length * width)
    score_scale = 1.0 / math.sqrt(HEAD_NOPE + ROPE)
    every_query = lax.all_gather(query, "heads", axis=2, tiled=True)
    all_heads = every_query.shape[2]
    row_count = QTOK * all_heads
    query_rows = every_query.reshape(seq_count, row_count, width)
    draft = jnp.arange(row_count, dtype=jnp.int32) // all_heads
    limits = lengths[:, None] - QTOK + draft[None, :]
    key_rows = local_keys.reshape(seq_count, half_length, width)
    highest, totals, mixed = partial_softmax(
        query_rows, key_rows, my_half * half_length, limits, score_scale
    )
    shaped = (
        highest.reshape(1, seq_count, QTOK, all_heads),
        totals.reshape(1, seq_count, QTOK, all_heads),
        mixed.reshape(1, seq_count, QTOK, all_heads, LATENT),
    )
    pieces = (
        lax.all_to_all(shaped[0], "heads", split_axis=3, concat_axis=0, tiled=True),
        lax.all_to_all(shaped[1], "heads", split_axis=3, concat_axis=0, tiled=True),
        lax.all_to_all(shaped[2], "heads", split_axis=3, concat_axis=0, tiled=True),
    )
    overall = jnp.max(pieces[0], axis=0)
    factor = jnp.exp(pieces[0] - overall[None])
    totals = jnp.sum(pieces[1] * factor, axis=0)
    mixed = jnp.sum(pieces[2] * factor[..., None], axis=0)
    context = (mixed / totals[..., None]).astype(jnp.bfloat16)
    return context


def send_orders(batch_count):
    whole = list(range(1, batch_count))
    if batch_count != 8:
        return [whole] * 4, [[0] + whole] * 4
    sends = [
        [1, 2, 3, 4, 5, 6, 7],
        [6, 1, 2, 3, 4, 5, 7],
        [6, 4, 5, 2, 3, 7, 1],
        [6, 7, 2, 3, 4, 5, 1],
    ]
    uses = [
        [0, 1, 2, 6, 4, 7, 5, 3],
        [0, 1, 2, 3, 6, 4, 5, 7],
        [0, 1, 6, 2, 4, 3, 5, 7],
        [0, 1, 2, 3, 4, 5, 6, 7],
    ]
    return sends, uses


def fused_kernel(
    batch_count, table_ref, length_ref, storage_ref, query_ref, out_ref,
    tabled, lengthy, stored, asked, outgoing, keys, queries, places, mixed,
    load_sem, fetch_sem, send_sem, recv_sem, pass_sem, take_sem, ready_sem,
):
    slot_count = stored.shape[0]
    per_peer = slot_count // batch_count
    block_count = MAXLEN // BLK
    width = LATENT + ROPE
    span = 2 * width
    pieces = BLK // 2
    me = lax.axis_index("batch")
    half = lax.axis_index("heads")
    sibling = 1 - half
    depth = me // 2
    deep = batch_count // 2
    left = depth == deep // 2 - 1
    right = depth == deep // 2
    middle = left | right
    across = batch_count - 2
    sends, uses = send_orders(batch_count)
    kind = jnp.where(left, 1, jnp.where(right, 2, jnp.where(depth < deep // 2, 0, 3)))

    def flip(step):
        other = me
        bit = 1
        while bit < batch_count:
            other = other + bit * (1 - 2 * ((me // bit) % 2)) * ((step // bit) % 2)
            bit *= 2
        return other

    def chosen(table, place):
        picked = table[3][place]
        for index in range(3):
            picked = jnp.where(kind == index, table[index][place], picked)
        return picked

    def columns(piece):
        return pl.ds(piece * span, span)

    def rows(index):
        return pl.ds(pl.multiple_of(index * per_peer, per_peer), per_peer)

    load_table = pltpu.make_async_copy(table_ref, tabled, load_sem.at[0])
    load_query = pltpu.make_async_copy(query_ref, asked, load_sem.at[1])
    load_length = pltpu.make_async_copy(length_ref, lengthy, load_sem.at[2])
    fetches = [
        pltpu.make_async_copy(
            storage_ref.at[:, columns(piece)], stored.at[:, columns(piece)], fetch_sem.at[piece]
        )
        for piece in range(pieces)
    ]
    load_table.start()
    for fetch in fetches:
        fetch.start()

    barrier = pltpu.get_barrier_semaphore()

    def tell(other, core):
        pl.semaphore_signal(
            barrier, inc=1, device_id={"batch": other, "heads": core}, device_id_type=MESH
        )

    @pl.when(middle)
    def _():
        tell(flip(across), half)

    for spot in range(batch_count):
        if spot // 2 in (deep // 2 - 1, deep // 2):
            continue
        for core in range(2):

            @pl.when((me != spot) | (half != core))
            def _():
                tell(spot, core)

    load_query.start()
    load_length.start()

    load_table.wait()
    table = tabled[...]
    row_ids = lax.broadcasted_iota(jnp.int32, table.shape, 0)
    square = (slot_count, slot_count)
    down = lax.broadcasted_iota(jnp.int32, square, 0)
    along = lax.broadcasted_iota(jnp.int32, square, 1)
    earlier = (down < along).astype(jnp.float32).astype(jnp.bfloat16)
    own = jnp.sum(jnp.where(row_ids == 2 * me + half, table, 0), axis=0, keepdims=True)
    owner = own // block_count
    belongs = (row_ids == owner).astype(jnp.float32)
    counts = jnp.dot(belongs.astype(jnp.bfloat16), earlier, preferred_element_type=jnp.float32)
    rank = jnp.sum(belongs * counts, axis=0, keepdims=True).astype(jnp.int32)
    place = owner * per_peer + rank
    order = (down == place).astype(jnp.float32).astype(jnp.bfloat16)

    lanes = lax.broadcasted_iota(jnp.int32, (1, 2 * ROPE), 1)
    first_lanes = (lanes < ROPE).astype(jnp.float32).astype(jnp.bfloat16)
    last_lanes = (lanes >= ROPE).astype(jnp.float32).astype(jnp.bfloat16)

    def group(piece):
        fetches[piece].wait()
        base = piece * span
        moved = jnp.dot(
            order, stored[:, columns(piece)], preferred_element_type=jnp.float32
        )
        outgoing[:, base : base + LATENT] = moved[:, :LATENT].astype(jnp.bfloat16)
        outgoing[:, base + LATENT : base + 2 * LATENT] = moved[
            :, width : width + LATENT
        ].astype(jnp.bfloat16)
        outgoing[:, base + 2 * LATENT : base + span] = jnp.where(
            lanes < ROPE, moved[:, LATENT : LATENT + 2 * ROPE], moved[:, span - 2 * ROPE :]
        ).astype(jnp.bfloat16)

    def send(step, where):
        other = flip(step)
        return pltpu.make_async_remote_copy(
            src_ref=outgoing.at[rows(other), where],
            dst_ref=keys.at[half, rows(me), where],
            send_sem=send_sem.at[step],
            recv_sem=recv_sem.at[step],
            device_id={"batch": other},
            device_id_type=MESH,
        )

    everything = pl.ds(0, pieces * span)

    def arrival(step):
        other = flip(step)
        return pltpu.make_async_remote_copy(
            src_ref=outgoing.at[rows(other), everything],
            dst_ref=keys.at[half, rows(other), everything],
            send_sem=send_sem.at[step],
            recv_sem=recv_sem.at[step],
            device_id={"batch": other},
            device_id_type=MESH,
        )

    def hand_over(step, source):
        other = flip(step)
        return pltpu.make_async_remote_copy(
            src_ref=source.at[rows(other)],
            dst_ref=keys.at[half, rows(other)],
            send_sem=pass_sem.at[step],
            recv_sem=take_sem.at[step],
            device_id={"heads": sibling},
            device_id_type=MESH,
        )

    for piece in range(pieces):
        group(piece)

        @pl.when(middle)
        def _():
            if piece == 0:
                pl.semaphore_wait(barrier, 1)
            send(across, columns(piece)).start()

    @pl.when(middle)
    def _():
        pl.semaphore_wait(ready_sem, 1)

    @pl.when(jnp.logical_not(middle))
    def _():
        pl.semaphore_wait(barrier, 2 * batch_count - 1)

        @pl.when((depth == 0) | (depth == deep - 1))
        def _():
            inner = jnp.where(depth == 0, me + batch_count - 2 - deep, me - batch_count + 2 + deep)
            pl.semaphore_signal(
                ready_sem, inc=1, device_id={"batch": inner}, device_id_type=MESH
            )

        send(chosen(sends, 0), everything).start()

    for turn in range(1, batch_count - 1):
        send(chosen(sends, turn), everything).start()
    hand_over(0, outgoing).start()

    keys[half, rows(me)] = outgoing[rows(me)]

    mine = table // block_count == me
    marks = mine.astype(jnp.float32)
    ranks = jnp.dot(
        marks.astype(jnp.bfloat16), earlier, preferred_element_type=jnp.float32
    ).astype(jnp.int32)
    ranks = jnp.where(mine, ranks, -1)
    blocks = (table % block_count).astype(jnp.float32)
    lane = lax.broadcasted_iota(jnp.int32, table.shape, 1)
    spots = (lane // per_peer).astype(jnp.float32)
    for index in range(per_peer):
        number = jnp.sum(jnp.where(ranks == index, blocks, 0.0), axis=1, keepdims=True)
        spots = spots + jnp.where(lane % per_peer == index, number * BLK, 0.0)
    places[...] = spots

    row_count = asked.shape[0]
    heads = row_count // QTOK
    load_length.wait()
    limits = [(lengthy[0] - QTOK + draft).astype(jnp.float32) for draft in range(QTOK)]

    load_query.wait()
    asking = asked[...]
    queries[:, :width] = asking
    queries[:, width:] = asking[:, LATENT:]

    factor = math.log2(math.e) / math.sqrt(HEAD_NOPE + ROPE)
    peak = jnp.full((row_count, 1), -1e30, jnp.float32)
    totals = jnp.zeros((row_count, slot_count), jnp.float32)
    steps = [0] + [chosen(uses, turn) for turn in range(1, batch_count)]
    for turn in range(batch_count):
        if turn + AHEAD < batch_count:
            for ahead in range(1 if turn == 0 else turn + AHEAD, turn + AHEAD + 1):
                arrival(steps[ahead]).wait_recv()
                hand_over(steps[ahead], keys.at[half]).start()
        step = steps[turn]
        other = me if turn == 0 else flip(step)
        hand_over(step, keys.at[half]).wait_recv()
        latents = []
        ropes = []
        for core in range(2):
            for piece in range(pieces):
                base = piece * span
                pair = keys[core, rows(other), base + 2 * LATENT : base + span]
                for parity in range(2):
                    low = base + parity * LATENT
                    latents.append(keys[core, rows(other), low : low + LATENT])
                    ropes.append(pair * (last_lanes if parity else first_lanes))
        latent = jnp.concatenate(latents, axis=0)
        rope = jnp.concatenate(ropes, axis=0)
        dots = lax.dot_general(
            queries[...],
            jnp.concatenate([latent, rope], axis=1),
            NT,
            preferred_element_type=jnp.float32,
        )
        at = places[pl.ds(2 * other, 2), :]
        at = jnp.concatenate([at[0:1], at[1:2]], axis=1)
        scores = jnp.concatenate(
            [
                dots[draft * heads : (draft + 1) * heads]
                + jnp.where(at <= limits[draft], 0.0, -1e30)
                for draft in range(QTOK)
            ],
            axis=0,
        )
        higher = jnp.maximum(peak, jnp.max(scores, axis=1, keepdims=True))
        raised = jnp.exp2((scores - higher) * factor)
        sums = raised[:, :slot_count] + raised[:, slot_count:]
        fresh = jnp.dot(raised.astype(jnp.bfloat16), latent, preferred_element_type=jnp.float32)
        if turn == 0:
            totals = sums
            mixed[...] = fresh
        else:
            shrink = jnp.exp2((peak - higher) * factor)
            totals = totals * shrink + sums
            mixed[...] = mixed[...] * shrink + fresh
        peak = higher
    total = jnp.sum(totals, axis=1, keepdims=True)
    out_ref[...] = (mixed[...] / total).astype(out_ref.dtype)
    for step in range(1, batch_count):
        send(step, everything).wait_send()
    for step in range(batch_count):
        hand_over(step, keys.at[half]).wait_send()


def local(storage, block_table, lengths, query):
    batch_count = lax.axis_size("batch")
    slot_count = storage.shape[1]
    per_peer = slot_count // batch_count
    whole = batch_count & (batch_count - 1) == 0 and query.shape[0] == SEQ_DEV
    whole = whole and batch_count >= 8 and lax.axis_size("heads") == 2
    if per_peer % 16 or slot_count != 128 or BLK * per_peer != slot_count or not whole:
        return plain_local(storage, block_table, lengths, query)
    width = LATENT + ROPE
    heads = query.shape[2]
    row_count = QTOK * heads
    vmem = pl.BlockSpec(memory_space=pltpu.VMEM)
    anywhere = pl.BlockSpec(memory_space=pltpu.HBM)
    context = pl.pallas_call(
        functools.partial(fused_kernel, batch_count),
        out_shape=jax.ShapeDtypeStruct((row_count, LATENT), jnp.bfloat16),
        in_specs=[anywhere] * 4,
        out_specs=vmem,
        scratch_shapes=[
            pltpu.VMEM((block_table.shape[0] // slot_count, slot_count), jnp.int32),
            pltpu.SMEM(lengths.shape, jnp.int32),
            pltpu.VMEM((slot_count, BLK * width), jnp.bfloat16),
            pltpu.VMEM((row_count, width), jnp.bfloat16),
            pltpu.VMEM((slot_count, BLK * width), jnp.bfloat16),
            pltpu.VMEM((2, slot_count, BLK * width), jnp.bfloat16),
            pltpu.VMEM((row_count, LATENT + 2 * ROPE), jnp.bfloat16),
            pltpu.VMEM((block_table.shape[0] // slot_count, slot_count), jnp.float32),
            pltpu.VMEM((row_count, LATENT), jnp.float32),
            pltpu.SemaphoreType.DMA((3,)),
            pltpu.SemaphoreType.DMA((BLK // 2,)),
            pltpu.SemaphoreType.DMA((batch_count,)),
            pltpu.SemaphoreType.DMA((batch_count,)),
            pltpu.SemaphoreType.DMA((batch_count,)),
            pltpu.SemaphoreType.DMA((batch_count,)),
            pltpu.SemaphoreType.REGULAR,
        ],
        compiler_params=pltpu.CompilerParams(collective_id=0, has_side_effects=True, vmem_limit_bytes=54800 * 1024),
    )(
        pltpu.with_memory_space_constraint(block_table.reshape(-1, slot_count), pltpu.HBM),
        lengths,
        storage[0],
        query.reshape(row_count, width),
    )
    return context.reshape(1, QTOK, heads, LATENT)


def solution(mesh):
    in_specs = (
        P(None, ("groups", "batch", "heads"), None),
        P("groups"),
        P(("groups", "batch")),
        P(("groups", "batch"), None, "heads", None),
    )
    out_specs = P(("groups", "batch"), None, "heads", None)
    return jax.shard_map(local, mesh=mesh, in_specs=in_specs, out_specs=out_specs, check_vma=False)
```

```python
import functools
import math

import jax
import jax.numpy as jnp
from jax import lax
from jax.experimental import pallas as pl
from jax.experimental.pallas import tpu as pltpu
from jax.sharding import PartitionSpec as P

MESH = pl.DeviceIdType.MESH
NT = (((1,), (1,)), ((), ()))
LATENT = 512
ROPE = 64
HEAD_NOPE = 128
SEQ_DEV = 1
MAXLEN = 2048
BLK = 8
QTOK = 4
SHARES = 1
AHEAD = 2
HOLDS = (3, 4)


def partial_softmax(query_rows, key_rows, first_place, limits, score_scale):
    scores = (
        jnp.einsum("src,stc->srt", query_rows, key_rows, preferred_element_type=jnp.float32)
        * score_scale
    )
    places = first_place + jnp.arange(key_rows.shape[1], dtype=jnp.int32)
    visible = places[None, None, :] <= limits[:, :, None]
    masked = jnp.where(visible, scores, -1e30)
    highest = jnp.max(masked, axis=2)
    raised = jnp.where(visible, jnp.exp(masked - highest[:, :, None]), 0.0)
    totals = jnp.sum(raised, axis=2)
    mixed = jnp.einsum(
        "srt,stc->src",
        raised.astype(jnp.bfloat16),
        key_rows[:, :, :LATENT],
        preferred_element_type=jnp.float32,
    )
    return (highest, totals, mixed)


def plain_local(storage, block_table, lengths, query):
    batch_count = lax.axis_size("batch")
    head_groups = lax.axis_size("heads")
    my_batch = lax.axis_index("batch")
    my_half = lax.axis_index("heads")
    slot_count = storage.shape[1]
    per_peer = slot_count // batch_count
    block_count = MAXLEN // BLK
    half_blocks = block_count // head_groups
    width = LATENT + ROPE
    zero_index = jnp.zeros((), jnp.int32)
    table_grid = block_table.reshape(batch_count, head_groups, slot_count)
    own_table = lax.dynamic_slice(
        table_grid, (my_batch, my_half, zero_index), (1, 1, slot_count)
    ).reshape(slot_count)
    owner = own_table // block_count // SEQ_DEV
    owner_table = (owner[:, None] == jnp.arange(batch_count, dtype=jnp.int32)[None, :]).astype(
        jnp.int32
    )
    rank = jnp.sum(owner_table * (jnp.cumsum(owner_table, axis=0) - 1), axis=1)
    send_place = owner * per_peer + rank
    order = (
        jnp.zeros((slot_count,), jnp.int32)
        .at[send_place]
        .set(jnp.arange(slot_count, dtype=jnp.int32))
    )
    outgoing = jnp.take(storage, order, axis=1)
    received = lax.all_to_all(outgoing, "batch", split_axis=1, concat_axis=1, tiled=True)
    sender_table = lax.dynamic_slice(
        table_grid, (zero_index, my_half, zero_index), (batch_count, 1, slot_count)
    ).reshape(batch_count, slot_count)
    sequence_ids = sender_table // block_count
    arrivals = sequence_ids // SEQ_DEV == my_batch
    arrive_place = (
        jnp.arange(batch_count, dtype=jnp.int32)[:, None] * per_peer
        + jnp.cumsum(arrivals.astype(jnp.int32), axis=1)
        - 1
    )
    target = (
        (sequence_ids - my_batch * SEQ_DEV) * half_blocks
        + sender_table % block_count
        - my_half * half_blocks
    )
    target = jnp.where(arrivals, target, slot_count)
    source = (
        jnp.zeros((slot_count,), jnp.int32)
        .at[target.reshape(-1)]
        .set(arrive_place.reshape(-1), mode="drop")
    )
    serving = jnp.take(received, source, axis=1)
    half_length = half_blocks * BLK
    seq_count = query.shape[0]
    local_keys = serving[0].reshape(seq_count, half_length * width)
    score_scale = 1.0 / math.sqrt(HEAD_NOPE + ROPE)
    every_query = lax.all_gather(query, "heads", axis=2, tiled=True)
    all_heads = every_query.shape[2]
    row_count = QTOK * all_heads
    query_rows = every_query.reshape(seq_count, row_count, width)
    draft = jnp.arange(row_count, dtype=jnp.int32) // all_heads
    limits = lengths[:, None] - QTOK + draft[None, :]
    key_rows = local_keys.reshape(seq_count, half_length, width)
    highest, totals, mixed = partial_softmax(
        query_rows, key_rows, my_half * half_length, limits, score_scale
    )
    shaped = (
        highest.reshape(1, seq_count, QTOK, all_heads),
        totals.reshape(1, seq_count, QTOK, all_heads),
        mixed.reshape(1, seq_count, QTOK, all_heads, LATENT),
    )
    pieces = (
        lax.all_to_all(shaped[0], "heads", split_axis=3, concat_axis=0, tiled=True),
        lax.all_to_all(shaped[1], "heads", split_axis=3, concat_axis=0, tiled=True),
        lax.all_to_all(shaped[2], "heads", split_axis=3, concat_axis=0, tiled=True),
    )
    overall = jnp.max(pieces[0], axis=0)
    factor = jnp.exp(pieces[0] - overall[None])
    totals = jnp.sum(pieces[1] * factor, axis=0)
    mixed = jnp.sum(pieces[2] * factor[..., None], axis=0)
    context = (mixed / totals[..., None]).astype(jnp.bfloat16)
    return context


def send_orders(batch_count):
    whole = list(range(1, batch_count))
    if batch_count != 8:
        return [whole] * 8, [[0] + whole] * 8
    sends = [
        [1, 2, 3, 4, 5, 6, 7],
        [1, 2, 3, 4, 5, 6, 7],
        [6, 1, 2, 3, 7, 4, 5],
        [6, 1, 2, 3, 7, 4, 5],
        [6, 4, 5, 2, 3, 7, 1],
        [6, 4, 5, 2, 3, 7, 1],
        [6, 7, 2, 3, 1, 4, 5],
        [6, 7, 2, 3, 1, 4, 5],
    ]
    uses = [
        [0, 1, 6, 7, 4, 2, 5, 3],
        [0, 1, 6, 7, 4, 2, 5, 3],
        [0, 1, 2, 3, 6, 4, 5, 7],
        [0, 1, 2, 3, 6, 4, 7, 5],
        [0, 1, 6, 2, 4, 3, 7, 5],
        [0, 1, 6, 2, 4, 3, 7, 5],
        [0, 1, 2, 3, 6, 7, 4, 5],
        [0, 1, 2, 3, 6, 7, 4, 5],
    ]
    return sends, uses


def fused_kernel(
    batch_count, table_ref, length_ref, storage_ref, query_ref, out_ref,
    tabled, lengthy, stored, asked, outgoing, keys, queries, places, mixed,
    load_sem, fetch_sem, send_sem, recv_sem, pass_sem, take_sem, ready_sem,
):
    slot_count = stored.shape[0]
    per_peer = slot_count // batch_count
    block_count = MAXLEN // BLK
    width = LATENT + ROPE
    span = 2 * width
    pieces = BLK // 2
    me = lax.axis_index("batch")
    half = lax.axis_index("heads")
    sibling = 1 - half
    depth = me // 2
    deep = batch_count // 2
    left = depth == deep // 2 - 1
    right = depth == deep // 2
    middle = left | right
    across = batch_count - 2
    sends, uses = send_orders(batch_count)
    stage = jnp.where(left, 1, jnp.where(right, 2, jnp.where(depth < deep // 2, 0, 3)))
    kind = 2 * stage + me % 2

    def flip(step):
        other = me
        bit = 1
        while bit < batch_count:
            other = other + bit * (1 - 2 * ((me // bit) % 2)) * ((step // bit) % 2)
            bit *= 2
        return other

    def chosen(table, place):
        picked = table[0][place]
        for index in range(1, len(table)):
            if table[index][place] != table[0][place]:
                picked = jnp.where(kind == index, table[index][place], picked)
        return picked

    def columns(piece):
        return pl.ds(piece * span, span)

    def rows(index):
        return pl.ds(pl.multiple_of(index * per_peer, per_peer), per_peer)

    load_table = pltpu.make_async_copy(table_ref, tabled, load_sem.at[0])
    load_query = pltpu.make_async_copy(query_ref, asked, load_sem.at[1])
    load_length = pltpu.make_async_copy(length_ref, lengthy, load_sem.at[2])
    fetches = [
        pltpu.make_async_copy(
            storage_ref.at[:, columns(piece)], stored.at[:, columns(piece)], fetch_sem.at[piece]
        )
        for piece in range(pieces)
    ]
    load_table.start()
    for fetch in fetches:
        fetch.start()

    barrier = pltpu.get_barrier_semaphore()

    def tell(other, core):
        pl.semaphore_signal(
            barrier, inc=1, device_id={"batch": other, "heads": core}, device_id_type=MESH
        )

    @pl.when(middle)
    def _():
        tell(flip(across), half)

    for spot in range(batch_count):
        if spot // 2 in (deep // 2 - 1, deep // 2):
            continue
        for core in range(2):

            @pl.when((me != spot) | (half != core))
            def _():
                tell(spot, core)

    load_query.start()
    load_length.start()

    load_table.wait()
    table = tabled[...]
    row_ids = lax.broadcasted_iota(jnp.int32, table.shape, 0)
    square = (slot_count, slot_count)
    down = lax.broadcasted_iota(jnp.int32, square, 0)
    along = lax.broadcasted_iota(jnp.int32, square, 1)
    earlier = (down < along).astype(jnp.float32).astype(jnp.bfloat16)
    own = jnp.sum(jnp.where(row_ids == 2 * me + half, table, 0), axis=0, keepdims=True)
    owner = jnp.right_shift(own, block_count.bit_length() - 1)
    belongs = (row_ids == owner).astype(jnp.float32)
    counts = jnp.dot(belongs.astype(jnp.bfloat16), earlier, preferred_element_type=jnp.float32)
    rank = jnp.sum(belongs * counts, axis=0, keepdims=True).astype(jnp.int32)
    place = owner * per_peer + rank
    order = (down == place).astype(jnp.float32).astype(jnp.bfloat16)

    lanes = lax.broadcasted_iota(jnp.int32, (1, 2 * ROPE), 1)
    first_lanes = (lanes < ROPE).astype(jnp.float32).astype(jnp.bfloat16)
    last_lanes = (lanes >= ROPE).astype(jnp.float32).astype(jnp.bfloat16)

    def group(piece):
        fetches[piece].wait()
        base = piece * span
        moved = jnp.dot(
            order, stored[:, columns(piece)], preferred_element_type=jnp.float32
        )
        outgoing[:, base : base + LATENT] = moved[:, :LATENT].astype(jnp.bfloat16)
        outgoing[:, base + LATENT : base + 2 * LATENT] = moved[
            :, width : width + LATENT
        ].astype(jnp.bfloat16)
        outgoing[:, base + 2 * LATENT : base + span] = jnp.where(
            lanes < ROPE, moved[:, LATENT : LATENT + 2 * ROPE], moved[:, span - 2 * ROPE :]
        ).astype(jnp.bfloat16)

    def send(step, where):
        other = flip(step)
        return pltpu.make_async_remote_copy(
            src_ref=outgoing.at[rows(other), where],
            dst_ref=keys.at[half, rows(me), where],
            send_sem=send_sem,
            recv_sem=recv_sem.at[step - 1],
            device_id={"batch": other},
            device_id_type=MESH,
        )

    everything = pl.ds(0, pieces * span)

    def arrival(step):
        other = flip(step)
        return pltpu.make_async_remote_copy(
            src_ref=outgoing.at[rows(other), everything],
            dst_ref=keys.at[half, rows(other), everything],
            send_sem=send_sem,
            recv_sem=recv_sem.at[step - 1],
            device_id={"batch": other},
            device_id_type=MESH,
        )

    def hand_over(step, source):
        other = flip(step)
        return pltpu.make_async_remote_copy(
            src_ref=source.at[rows(other)],
            dst_ref=keys.at[half, rows(other)],
            send_sem=pass_sem,
            recv_sem=take_sem.at[step],
            device_id={"heads": sibling},
            device_id_type=MESH,
        )

    for piece in range(pieces):
        group(piece)

        @pl.when(middle)
        def _():
            if piece == 0:
                pl.semaphore_wait(barrier, 1)
            send(across, columns(piece)).start()

    @pl.when(middle)
    def _():
        pl.semaphore_wait(ready_sem, 1)

    @pl.when(jnp.logical_not(middle))
    def _():
        pl.semaphore_wait(barrier, 2 * batch_count - 1)

        @pl.when((depth == 0) | (depth == deep - 1))
        def _():
            inner = jnp.where(depth == 0, me + batch_count - 2 - deep, me - batch_count + 2 + deep)
            pl.semaphore_signal(
                ready_sem, inc=1, device_id={"batch": inner}, device_id_type=MESH
            )

        send(chosen(sends, 0), everything).start()

    for turn in range(1, batch_count - 3):
        send(chosen(sends, turn), everything).start()

    held = depth == deep - 1

    def send_late(late):
        send(chosen(sends, batch_count - 3 + late), everything).start()

    @pl.when(jnp.logical_not(held))
    def _():
        for late in range(2):
            send_late(late)

    hand_over(0, outgoing).start()

    keys[half, rows(me)] = outgoing[rows(me)]

    mine = jnp.right_shift(table, block_count.bit_length() - 1) == me
    marks = mine.astype(jnp.float32)
    ranks = jnp.dot(
        marks.astype(jnp.bfloat16), earlier, preferred_element_type=jnp.float32
    ).astype(jnp.int32)
    ranks = jnp.where(mine, ranks, -1)
    blocks = jnp.bitwise_and(table, block_count - 1).astype(jnp.float32)
    lane = lax.broadcasted_iota(jnp.int32, table.shape, 1)
    spots = (lane // per_peer).astype(jnp.float32)
    for index in range(per_peer):
        number = jnp.sum(jnp.where(ranks == index, blocks, 0.0), axis=1, keepdims=True)
        spots = spots + jnp.where(lane % per_peer == index, number * BLK, 0.0)
    places[...] = spots

    row_count = asked.shape[0]
    heads = row_count // QTOK
    load_length.wait()
    limits = [(lengthy[0] - QTOK + draft).astype(jnp.float32) for draft in range(QTOK)]

    load_query.wait()
    asking = asked[...]
    queries[:, :width] = asking
    queries[:, width:] = asking[:, LATENT:]

    factor = math.log2(math.e) / math.sqrt(HEAD_NOPE + ROPE)
    portion = row_count // SHARES
    peaks = [jnp.full((portion, 1), -1e30, jnp.float32)] * SHARES
    totals = [None] * SHARES
    steps = [0] + [chosen(uses, turn) for turn in range(1, batch_count)]
    for turn in range(batch_count):
        if turn + AHEAD < batch_count:
            for ahead in range(1 if turn == 0 else turn + AHEAD, turn + AHEAD + 1):
                arrival(steps[ahead]).wait_recv()
                if ahead in HOLDS:

                    @pl.when(held)
                    def _():
                        send_late(HOLDS.index(ahead))

                hand_over(steps[ahead], keys.at[half]).start()
        step = steps[turn]
        other = me if turn == 0 else flip(step)
        hand_over(step, keys.at[half]).wait_recv()
        latents = []
        ropes = []
        for core in range(2):
            for piece in range(pieces):
                base = piece * span
                pair = keys[core, rows(other), base + 2 * LATENT : base + span]
                for parity in range(2):
                    low = base + parity * LATENT
                    latents.append(keys[core, rows(other), low : low + LATENT])
                    ropes.append(pair * (last_lanes if parity else first_lanes))
        latent = jnp.concatenate(latents, axis=0)
        rope = jnp.concatenate(ropes, axis=0)
        whole = jnp.concatenate([latent, rope], axis=1)
        at = places[pl.ds(2 * other, 2), :]
        at = jnp.concatenate([at[0:1], at[1:2]], axis=1)
        masks = [jnp.where(at <= limits[draft], 0.0, -1e30) for draft in range(QTOK)]
        for share in range(SHARES):
            low, high = share * portion, (share + 1) * portion
            dots = lax.dot_general(
                queries[low:high], whole, NT, preferred_element_type=jnp.float32
            )
            scores = jnp.concatenate(
                [
                    dots[draft * heads - low : (draft + 1) * heads - low] + masks[draft]
                    for draft in range(low // heads, high // heads)
                ],
                axis=0,
            )
            higher = jnp.maximum(peaks[share], jnp.max(scores, axis=1, keepdims=True))
            raised = jnp.exp2((scores - higher) * factor)
            sums = raised[:, :slot_count] + raised[:, slot_count:]
            fresh = jnp.dot(
                raised.astype(jnp.bfloat16), latent, preferred_element_type=jnp.float32
            )
            if turn == 0:
                totals[share] = sums
                mixed[low:high] = fresh
            else:
                shrink = jnp.exp2((peaks[share] - higher) * factor)
                totals[share] = totals[share] * shrink + sums
                mixed[low:high] = mixed[low:high] * shrink + fresh
            peaks[share] = higher
    for share in range(SHARES):
        low, high = share * portion, (share + 1) * portion
        inverse = 1.0 / jnp.sum(totals[share], axis=1, keepdims=True)
        out_ref[low:high] = (mixed[low:high] * inverse).astype(out_ref.dtype)
    others = pl.ds(0, slot_count - per_peer)
    pltpu.make_async_remote_copy(
        src_ref=outgoing.at[others],
        dst_ref=keys.at[half, others],
        send_sem=send_sem,
        recv_sem=recv_sem.at[0],
        device_id={"heads": sibling},
        device_id_type=MESH,
    ).wait_send()
    pltpu.make_async_remote_copy(
        src_ref=keys.at[half],
        dst_ref=keys.at[half],
        send_sem=pass_sem,
        recv_sem=take_sem.at[0],
        device_id={"heads": sibling},
        device_id_type=MESH,
    ).wait_send()


def local(storage, block_table, lengths, query):
    batch_count = lax.axis_size("batch")
    slot_count = storage.shape[1]
    per_peer = slot_count // batch_count
    whole = batch_count & (batch_count - 1) == 0 and query.shape[0] == SEQ_DEV
    whole = whole and batch_count >= 8 and lax.axis_size("heads") == 2
    if per_peer % 16 or slot_count != 128 or BLK * per_peer != slot_count or not whole:
        return plain_local(storage, block_table, lengths, query)
    width = LATENT + ROPE
    heads = query.shape[2]
    row_count = QTOK * heads
    vmem = pl.BlockSpec(memory_space=pltpu.VMEM)
    anywhere = pl.BlockSpec(memory_space=pltpu.HBM)
    context = pl.pallas_call(
        functools.partial(fused_kernel, batch_count),
        out_shape=jax.ShapeDtypeStruct((row_count, LATENT), jnp.bfloat16),
        in_specs=[anywhere] * 4,
        out_specs=vmem,
        scratch_shapes=[
            pltpu.VMEM((block_table.shape[0] // slot_count, slot_count), jnp.int32),
            pltpu.SMEM(lengths.shape, jnp.int32),
            pltpu.VMEM((slot_count, BLK * width), jnp.bfloat16),
            pltpu.VMEM((row_count, width), jnp.bfloat16),
            pltpu.VMEM((slot_count, BLK * width), jnp.bfloat16),
            pltpu.VMEM((2, slot_count, BLK * width), jnp.bfloat16),
            pltpu.VMEM((row_count, LATENT + 2 * ROPE), jnp.bfloat16),
            pltpu.VMEM((block_table.shape[0] // slot_count, slot_count), jnp.float32),
            pltpu.VMEM((row_count, LATENT), jnp.float32),
            pltpu.SemaphoreType.DMA((3,)),
            pltpu.SemaphoreType.DMA((BLK // 2,)),
            pltpu.SemaphoreType.DMA,
            pltpu.SemaphoreType.DMA((batch_count - 1,)),
            pltpu.SemaphoreType.DMA,
            pltpu.SemaphoreType.DMA((batch_count,)),
            pltpu.SemaphoreType.REGULAR,
        ],
        compiler_params=pltpu.CompilerParams(collective_id=0, has_side_effects=True, vmem_limit_bytes=54800 * 1024),
    )(
        pltpu.with_memory_space_constraint(block_table.reshape(-1, slot_count), pltpu.HBM),
        lengths,
        storage[0],
        query.reshape(row_count, width),
    )
    return context.reshape(1, QTOK, heads, LATENT)


def solution(mesh):
    in_specs = (
        P(None, ("groups", "batch", "heads"), None),
        P("groups"),
        P(("groups", "batch")),
        P(("groups", "batch"), None, "heads", None),
    )
    out_specs = P(("groups", "batch"), None, "heads", None)
    return jax.shard_map(local, mesh=mesh, in_specs=in_specs, out_specs=out_specs, check_vma=False)
```

```python
import functools
import math

import jax
import jax.numpy as jnp
from jax import lax
from jax.experimental import pallas as pl
from jax.experimental.pallas import tpu as pltpu
from jax.sharding import PartitionSpec as P

MESH = pl.DeviceIdType.MESH
NT = (((1,), (1,)), ((), ()))
LATENT = 512
ROPE = 64
HEAD_NOPE = 128
SEQ_DEV = 1
MAXLEN = 2048
BLK = 8
QTOK = 4
SHARES = 1
AHEAD = 2
HOLDS = (3, 4)


def partial_softmax(query_rows, key_rows, first_place, limits, score_scale):
    scores = (
        jnp.einsum("src,stc->srt", query_rows, key_rows, preferred_element_type=jnp.float32)
        * score_scale
    )
    places = first_place + jnp.arange(key_rows.shape[1], dtype=jnp.int32)
    visible = places[None, None, :] <= limits[:, :, None]
    masked = jnp.where(visible, scores, -1e30)
    highest = jnp.max(masked, axis=2)
    raised = jnp.where(visible, jnp.exp(masked - highest[:, :, None]), 0.0)
    totals = jnp.sum(raised, axis=2)
    mixed = jnp.einsum(
        "srt,stc->src",
        raised.astype(jnp.bfloat16),
        key_rows[:, :, :LATENT],
        preferred_element_type=jnp.float32,
    )
    return (highest, totals, mixed)


def plain_local(storage, block_table, lengths, query):
    batch_count = lax.axis_size("batch")
    head_groups = lax.axis_size("heads")
    my_batch = lax.axis_index("batch")
    my_half = lax.axis_index("heads")
    slot_count = storage.shape[1]
    per_peer = slot_count // batch_count
    block_count = MAXLEN // BLK
    half_blocks = block_count // head_groups
    width = LATENT + ROPE
    zero_index = jnp.zeros((), jnp.int32)
    table_grid = block_table.reshape(batch_count, head_groups, slot_count)
    own_table = lax.dynamic_slice(
        table_grid, (my_batch, my_half, zero_index), (1, 1, slot_count)
    ).reshape(slot_count)
    owner = own_table // block_count // SEQ_DEV
    owner_table = (owner[:, None] == jnp.arange(batch_count, dtype=jnp.int32)[None, :]).astype(
        jnp.int32
    )
    rank = jnp.sum(owner_table * (jnp.cumsum(owner_table, axis=0) - 1), axis=1)
    send_place = owner * per_peer + rank
    order = (
        jnp.zeros((slot_count,), jnp.int32)
        .at[send_place]
        .set(jnp.arange(slot_count, dtype=jnp.int32))
    )
    outgoing = jnp.take(storage, order, axis=1)
    received = lax.all_to_all(outgoing, "batch", split_axis=1, concat_axis=1, tiled=True)
    sender_table = lax.dynamic_slice(
        table_grid, (zero_index, my_half, zero_index), (batch_count, 1, slot_count)
    ).reshape(batch_count, slot_count)
    sequence_ids = sender_table // block_count
    arrivals = sequence_ids // SEQ_DEV == my_batch
    arrive_place = (
        jnp.arange(batch_count, dtype=jnp.int32)[:, None] * per_peer
        + jnp.cumsum(arrivals.astype(jnp.int32), axis=1)
        - 1
    )
    target = (
        (sequence_ids - my_batch * SEQ_DEV) * half_blocks
        + sender_table % block_count
        - my_half * half_blocks
    )
    target = jnp.where(arrivals, target, slot_count)
    source = (
        jnp.zeros((slot_count,), jnp.int32)
        .at[target.reshape(-1)]
        .set(arrive_place.reshape(-1), mode="drop")
    )
    serving = jnp.take(received, source, axis=1)
    half_length = half_blocks * BLK
    seq_count = query.shape[0]
    local_keys = serving[0].reshape(seq_count, half_length * width)
    score_scale = 1.0 / math.sqrt(HEAD_NOPE + ROPE)
    every_query = lax.all_gather(query, "heads", axis=2, tiled=True)
    all_heads = every_query.shape[2]
    row_count = QTOK * all_heads
    query_rows = every_query.reshape(seq_count, row_count, width)
    draft = jnp.arange(row_count, dtype=jnp.int32) // all_heads
    limits = lengths[:, None] - QTOK + draft[None, :]
    key_rows = local_keys.reshape(seq_count, half_length, width)
    highest, totals, mixed = partial_softmax(
        query_rows, key_rows, my_half * half_length, limits, score_scale
    )
    shaped = (
        highest.reshape(1, seq_count, QTOK, all_heads),
        totals.reshape(1, seq_count, QTOK, all_heads),
        mixed.reshape(1, seq_count, QTOK, all_heads, LATENT),
    )
    pieces = (
        lax.all_to_all(shaped[0], "heads", split_axis=3, concat_axis=0, tiled=True),
        lax.all_to_all(shaped[1], "heads", split_axis=3, concat_axis=0, tiled=True),
        lax.all_to_all(shaped[2], "heads", split_axis=3, concat_axis=0, tiled=True),
    )
    overall = jnp.max(pieces[0], axis=0)
    factor = jnp.exp(pieces[0] - overall[None])
    totals = jnp.sum(pieces[1] * factor, axis=0)
    mixed = jnp.sum(pieces[2] * factor[..., None], axis=0)
    context = (mixed / totals[..., None]).astype(jnp.bfloat16)
    return context


def send_orders(batch_count):
    whole = list(range(1, batch_count))
    if batch_count != 8:
        return [whole] * 8, [[0] + whole] * 8
    sends = [
        [1, 2, 3, 4, 5, 6, 7],
        [1, 2, 3, 4, 5, 6, 7],
        [7, 1, 2, 3, 6, 4, 5],
        [7, 1, 2, 3, 6, 4, 5],
        [7, 4, 5, 2, 3, 6, 1],
        [7, 4, 5, 2, 3, 6, 1],
        [6, 7, 2, 3, 1, 4, 5],
        [6, 7, 2, 3, 1, 4, 5],
    ]
    uses = [
        [0, 1, 6, 7, 4, 2, 5, 3],
        [0, 1, 6, 7, 4, 2, 5, 3],
        [0, 1, 2, 3, 7, 4, 5, 6],
        [0, 1, 2, 3, 7, 4, 6, 5],
        [0, 1, 7, 2, 4, 3, 6, 5],
        [0, 1, 7, 2, 4, 3, 6, 5],
        [0, 1, 2, 3, 6, 7, 4, 5],
        [0, 1, 2, 3, 6, 7, 4, 5],
    ]
    return sends, uses


def fused_kernel(
    batch_count, table_ref, length_ref, storage_ref, query_ref, out_ref,
    tabled, lengthy, stored, asked, outgoing, keys, queries, places, mixed,
    load_sem, fetch_sem, send_sem, recv_sem, pass_sem, take_sem, ready_sem, ahead_of,
):
    slot_count = stored.shape[0]
    per_peer = slot_count // batch_count
    block_count = MAXLEN // BLK
    width = LATENT + ROPE
    span = 2 * width
    pieces = BLK // 2
    me = lax.axis_index("batch")
    half = lax.axis_index("heads")
    sibling = 1 - half
    depth = me // 2
    deep = batch_count // 2
    left = depth == deep // 2 - 1
    right = depth == deep // 2
    middle = left | right
    across = batch_count - 1
    sends, uses = send_orders(batch_count)
    stage = jnp.where(left, 1, jnp.where(right, 2, jnp.where(depth < deep // 2, 0, 3)))
    kind = 2 * stage + me % 2

    def flip(step):
        other = me
        bit = 1
        while bit < batch_count:
            other = other + bit * (1 - 2 * ((me // bit) % 2)) * ((step // bit) % 2)
            bit *= 2
        return other

    def chosen(table, place):
        picked = table[0][place]
        for index in range(1, len(table)):
            if table[index][place] != table[0][place]:
                picked = jnp.where(kind == index, table[index][place], picked)
        return picked

    def columns(piece):
        return pl.ds(piece * span, span)

    def rows(index):
        return pl.ds(pl.multiple_of(index * per_peer, per_peer), per_peer)

    load_table = pltpu.make_async_copy(table_ref, tabled, load_sem.at[0])
    load_query = pltpu.make_async_copy(query_ref, asked, load_sem.at[1])
    load_length = pltpu.make_async_copy(length_ref, lengthy, load_sem.at[2])
    fetches = [
        pltpu.make_async_copy(
            storage_ref.at[:, columns(piece)], stored.at[:, columns(piece)], fetch_sem.at[piece]
        )
        for piece in range(pieces)
    ]
    load_table.start()
    for fetch in fetches:
        fetch.start()

    barrier = pltpu.get_barrier_semaphore()

    def tell(other, core):
        pl.semaphore_signal(
            barrier, inc=1, device_id={"batch": other, "heads": core}, device_id_type=MESH
        )

    @pl.when(middle)
    def _():
        tell(flip(across), half)

    for spot in range(batch_count):
        if spot // 2 in (deep // 2 - 1, deep // 2):
            continue
        for core in range(2):

            @pl.when((me != spot) | (half != core))
            def _():
                tell(spot, core)

    load_query.start()
    load_length.start()

    load_table.wait()
    table = tabled[...]
    row_ids = lax.broadcasted_iota(jnp.int32, table.shape, 0)
    square = (slot_count, slot_count)
    down = lax.broadcasted_iota(jnp.int32, square, 0)
    along = lax.broadcasted_iota(jnp.int32, square, 1)
    earlier = (down < along).astype(jnp.float32).astype(jnp.bfloat16)
    own = jnp.sum(jnp.where(row_ids == 2 * me + half, table, 0), axis=0, keepdims=True)
    owner = jnp.right_shift(own, block_count.bit_length() - 1)
    belongs = (row_ids == owner).astype(jnp.float32)
    counts = jnp.dot(belongs.astype(jnp.bfloat16), earlier, preferred_element_type=jnp.float32)
    rank = jnp.sum(belongs * counts, axis=0, keepdims=True).astype(jnp.int32)
    place = owner * per_peer + rank
    order = (down == place).astype(jnp.float32).astype(jnp.bfloat16)

    lanes = lax.broadcasted_iota(jnp.int32, (1, 2 * ROPE), 1)
    first_lanes = (lanes < ROPE).astype(jnp.float32).astype(jnp.bfloat16)
    last_lanes = (lanes >= ROPE).astype(jnp.float32).astype(jnp.bfloat16)

    def gather(picks, piece, target, base):
        moved = jnp.dot(picks, stored[:, columns(piece)], preferred_element_type=jnp.float32)
        target[:, base : base + LATENT] = moved[:, :LATENT].astype(jnp.bfloat16)
        target[:, base + LATENT : base + 2 * LATENT] = moved[
            :, width : width + LATENT
        ].astype(jnp.bfloat16)
        target[:, base + 2 * LATENT : base + span] = jnp.where(
            lanes < ROPE, moved[:, LATENT : LATENT + 2 * ROPE], moved[:, span - 2 * ROPE :]
        ).astype(jnp.bfloat16)

    def send(step, where):
        other = flip(step)
        return pltpu.make_async_remote_copy(
            src_ref=outgoing.at[rows(other), where],
            dst_ref=keys.at[half, rows(me), where],
            send_sem=send_sem,
            recv_sem=recv_sem.at[step - 1],
            device_id={"batch": other},
            device_id_type=MESH,
        )

    everything = pl.ds(0, pieces * span)

    def arrival(step):
        other = flip(step)
        return pltpu.make_async_remote_copy(
            src_ref=outgoing.at[rows(other), everything],
            dst_ref=keys.at[half, rows(other), everything],
            send_sem=send_sem,
            recv_sem=recv_sem.at[step - 1],
            device_id={"batch": other},
            device_id_type=MESH,
        )

    def hand_over(step, source):
        other = flip(step)
        return pltpu.make_async_remote_copy(
            src_ref=source.at[rows(other)],
            dst_ref=keys.at[half, rows(other)],
            send_sem=pass_sem,
            recv_sem=take_sem.at[step],
            device_id={"heads": sibling},
            device_id_type=MESH,
        )

    fetches[0].wait()

    @pl.when(middle)
    def _():
        beside = lax.broadcasted_iota(jnp.int32, (per_peer, slot_count), 0)
        picks = beside + flip(across) * per_peer == place
        gather(picks.astype(jnp.float32).astype(jnp.bfloat16), 0, ahead_of, 0)
        pl.semaphore_wait(barrier, 1)
        pltpu.make_async_remote_copy(
            src_ref=ahead_of,
            dst_ref=keys.at[half, rows(me), columns(0)],
            send_sem=send_sem,
            recv_sem=recv_sem.at[across - 1],
            device_id={"batch": flip(across)},
            device_id_type=MESH,
        ).start()

    for piece in list(range(1, pieces)) + [0]:
        if piece:
            fetches[piece].wait()
        gather(order, piece, outgoing, piece * span)
        if piece:

            @pl.when(middle)
            def _():
                send(across, columns(piece)).start()

    @pl.when(middle)
    def _():
        pl.semaphore_wait(ready_sem, 1)

    @pl.when(jnp.logical_not(middle))
    def _():
        pl.semaphore_wait(barrier, 2 * batch_count - 1)

        @pl.when((depth == 0) | (depth == deep - 1))
        def _():
            inner = jnp.where(depth == 0, me + batch_count - 2 - deep, me - batch_count + 2 + deep)
            pl.semaphore_signal(
                ready_sem, inc=1, device_id={"batch": inner}, device_id_type=MESH
            )

        send(chosen(sends, 0), everything).start()

    for turn in range(1, batch_count - 3):
        send(chosen(sends, turn), everything).start()

    held = depth == deep - 1

    def send_late(late):
        send(chosen(sends, batch_count - 3 + late), everything).start()

    @pl.when(jnp.logical_not(held))
    def _():
        for late in range(2):
            send_late(late)

    hand_over(0, outgoing).start()

    keys[half, rows(me)] = outgoing[rows(me)]

    mine = jnp.right_shift(table, block_count.bit_length() - 1) == me
    marks = mine.astype(jnp.float32)
    ranks = jnp.dot(
        marks.astype(jnp.bfloat16), earlier, preferred_element_type=jnp.float32
    ).astype(jnp.int32)
    ranks = jnp.where(mine, ranks, -1)
    blocks = jnp.bitwise_and(table, block_count - 1).astype(jnp.float32)
    lane = lax.broadcasted_iota(jnp.int32, table.shape, 1)
    spots = (lane // per_peer).astype(jnp.float32)
    for index in range(per_peer):
        number = jnp.sum(jnp.where(ranks == index, blocks, 0.0), axis=1, keepdims=True)
        spots = spots + jnp.where(lane % per_peer == index, number * BLK, 0.0)
    places[...] = spots

    row_count = asked.shape[0]
    heads = row_count // QTOK
    load_length.wait()
    limits = [(lengthy[0] - QTOK + draft).astype(jnp.float32) for draft in range(QTOK)]

    load_query.wait()
    asking = asked[...]
    queries[:, :width] = asking
    queries[:, width:] = asking[:, LATENT:]

    factor = math.log2(math.e) / math.sqrt(HEAD_NOPE + ROPE)
    portion = row_count // SHARES
    peaks = [jnp.full((portion, 1), -1e30, jnp.float32)] * SHARES
    totals = [None] * SHARES
    steps = [0] + [chosen(uses, turn) for turn in range(1, batch_count)]
    for turn in range(batch_count):
        if turn + AHEAD < batch_count:
            for ahead in range(1 if turn == 0 else turn + AHEAD, turn + AHEAD + 1):
                arrival(steps[ahead]).wait_recv()
                if ahead in HOLDS:

                    @pl.when(held)
                    def _():
                        send_late(HOLDS.index(ahead))

                hand_over(steps[ahead], keys.at[half]).start()
        step = steps[turn]
        other = me if turn == 0 else flip(step)
        hand_over(step, keys.at[half]).wait_recv()
        latents = []
        ropes = []
        for core in range(2):
            for piece in range(pieces):
                base = piece * span
                pair = keys[core, rows(other), base + 2 * LATENT : base + span]
                for parity in range(2):
                    low = base + parity * LATENT
                    latents.append(keys[core, rows(other), low : low + LATENT])
                    ropes.append(pair * (last_lanes if parity else first_lanes))
        latent = jnp.concatenate(latents, axis=0)
        rope = jnp.concatenate(ropes, axis=0)
        whole = jnp.concatenate([latent, rope], axis=1)
        at = places[pl.ds(2 * other, 2), :]
        at = jnp.concatenate([at[0:1], at[1:2]], axis=1)
        masks = [jnp.where(at <= limits[draft], 0.0, -1e30) for draft in range(QTOK)]
        for share in range(SHARES):
            low, high = share * portion, (share + 1) * portion
            dots = lax.dot_general(
                queries[low:high], whole, NT, preferred_element_type=jnp.float32
            )
            scores = jnp.concatenate(
                [
                    dots[draft * heads - low : (draft + 1) * heads - low] + masks[draft]
                    for draft in range(low // heads, high // heads)
                ],
                axis=0,
            )
            higher = jnp.maximum(peaks[share], jnp.max(scores, axis=1, keepdims=True))
            raised = jnp.exp2((scores - higher) * factor)
            sums = raised[:, :slot_count] + raised[:, slot_count:]
            fresh = jnp.dot(
                raised.astype(jnp.bfloat16), latent, preferred_element_type=jnp.float32
            )
            if turn == 0:
                totals[share] = sums
                mixed[low:high] = fresh
            else:
                shrink = jnp.exp2((peaks[share] - higher) * factor)
                totals[share] = totals[share] * shrink + sums
                mixed[low:high] = mixed[low:high] * shrink + fresh
            peaks[share] = higher
    for share in range(SHARES):
        low, high = share * portion, (share + 1) * portion
        inverse = 1.0 / jnp.sum(totals[share], axis=1, keepdims=True)
        out_ref[low:high] = (mixed[low:high] * inverse).astype(out_ref.dtype)
    others = pl.ds(0, slot_count - per_peer)
    pltpu.make_async_remote_copy(
        src_ref=outgoing.at[others],
        dst_ref=keys.at[half, others],
        send_sem=send_sem,
        recv_sem=recv_sem.at[0],
        device_id={"heads": sibling},
        device_id_type=MESH,
    ).wait_send()
    pltpu.make_async_remote_copy(
        src_ref=keys.at[half],
        dst_ref=keys.at[half],
        send_sem=pass_sem,
        recv_sem=take_sem.at[0],
        device_id={"heads": sibling},
        device_id_type=MESH,
    ).wait_send()


def local(storage, block_table, lengths, query):
    batch_count = lax.axis_size("batch")
    slot_count = storage.shape[1]
    per_peer = slot_count // batch_count
    whole = batch_count & (batch_count - 1) == 0 and query.shape[0] == SEQ_DEV
    whole = whole and batch_count >= 8 and lax.axis_size("heads") == 2
    if per_peer % 16 or slot_count != 128 or BLK * per_peer != slot_count or not whole:
        return plain_local(storage, block_table, lengths, query)
    width = LATENT + ROPE
    heads = query.shape[2]
    row_count = QTOK * heads
    vmem = pl.BlockSpec(memory_space=pltpu.VMEM)
    anywhere = pl.BlockSpec(memory_space=pltpu.HBM)
    context = pl.pallas_call(
        functools.partial(fused_kernel, batch_count),
        out_shape=jax.ShapeDtypeStruct((row_count, LATENT), jnp.bfloat16),
        in_specs=[anywhere] * 4,
        out_specs=vmem,
        scratch_shapes=[
            pltpu.VMEM((block_table.shape[0] // slot_count, slot_count), jnp.int32),
            pltpu.SMEM(lengths.shape, jnp.int32),
            pltpu.VMEM((slot_count, BLK * width), jnp.bfloat16),
            pltpu.VMEM((row_count, width), jnp.bfloat16),
            pltpu.VMEM((slot_count, BLK * width), jnp.bfloat16),
            pltpu.VMEM((2, slot_count, BLK * width), jnp.bfloat16),
            pltpu.VMEM((row_count, LATENT + 2 * ROPE), jnp.bfloat16),
            pltpu.VMEM((block_table.shape[0] // slot_count, slot_count), jnp.float32),
            pltpu.VMEM((row_count, LATENT), jnp.float32),
            pltpu.SemaphoreType.DMA((3,)),
            pltpu.SemaphoreType.DMA((BLK // 2,)),
            pltpu.SemaphoreType.DMA,
            pltpu.SemaphoreType.DMA((batch_count - 1,)),
            pltpu.SemaphoreType.DMA,
            pltpu.SemaphoreType.DMA((batch_count,)),
            pltpu.SemaphoreType.REGULAR,
            pltpu.VMEM((per_peer, 2 * width), jnp.bfloat16),
        ],
        compiler_params=pltpu.CompilerParams(collective_id=0, has_side_effects=True, vmem_limit_bytes=54800 * 1024),
    )(
        pltpu.with_memory_space_constraint(block_table.reshape(-1, slot_count), pltpu.HBM),
        lengths,
        storage[0],
        query.reshape(row_count, width),
    )
    return context.reshape(1, QTOK, heads, LATENT)


def solution(mesh):
    in_specs = (
        P(None, ("groups", "batch", "heads"), None),
        P("groups"),
        P(("groups", "batch")),
        P(("groups", "batch"), None, "heads", None),
    )
    out_specs = P(("groups", "batch"), None, "heads", None)
    return jax.shard_map(local, mesh=mesh, in_specs=in_specs, out_specs=out_specs, check_vma=False)
```

```python
import functools
import math

import jax
import jax.numpy as jnp
from jax import lax
from jax.experimental import pallas as pl
from jax.experimental.pallas import tpu as pltpu
from jax.sharding import PartitionSpec as P

MESH = pl.DeviceIdType.MESH
NT = (((1,), (1,)), ((), ()))
LATENT = 512
ROPE = 64
HEAD_NOPE = 128
SEQ_DEV = 1
MAXLEN = 2048
BLK = 8
QTOK = 4
SHARES = 1
AHEAD = 2
HOLDS = (3, 4)


def partial_softmax(query_rows, key_rows, first_place, limits, score_scale):
    scores = (
        jnp.einsum("src,stc->srt", query_rows, key_rows, preferred_element_type=jnp.float32)
        * score_scale
    )
    places = first_place + jnp.arange(key_rows.shape[1], dtype=jnp.int32)
    visible = places[None, None, :] <= limits[:, :, None]
    masked = jnp.where(visible, scores, -1e30)
    highest = jnp.max(masked, axis=2)
    raised = jnp.where(visible, jnp.exp(masked - highest[:, :, None]), 0.0)
    totals = jnp.sum(raised, axis=2)
    mixed = jnp.einsum(
        "srt,stc->src",
        raised.astype(jnp.bfloat16),
        key_rows[:, :, :LATENT],
        preferred_element_type=jnp.float32,
    )
    return (highest, totals, mixed)


def plain_local(storage, block_table, lengths, query):
    batch_count = lax.axis_size("batch")
    head_groups = lax.axis_size("heads")
    my_batch = lax.axis_index("batch")
    my_half = lax.axis_index("heads")
    slot_count = storage.shape[1]
    per_peer = slot_count // batch_count
    block_count = MAXLEN // BLK
    half_blocks = block_count // head_groups
    width = LATENT + ROPE
    zero_index = jnp.zeros((), jnp.int32)
    table_grid = block_table.reshape(batch_count, head_groups, slot_count)
    own_table = lax.dynamic_slice(
        table_grid, (my_batch, my_half, zero_index), (1, 1, slot_count)
    ).reshape(slot_count)
    owner = own_table // block_count // SEQ_DEV
    owner_table = (owner[:, None] == jnp.arange(batch_count, dtype=jnp.int32)[None, :]).astype(
        jnp.int32
    )
    rank = jnp.sum(owner_table * (jnp.cumsum(owner_table, axis=0) - 1), axis=1)
    send_place = owner * per_peer + rank
    order = (
        jnp.zeros((slot_count,), jnp.int32)
        .at[send_place]
        .set(jnp.arange(slot_count, dtype=jnp.int32))
    )
    outgoing = jnp.take(storage, order, axis=1)
    received = lax.all_to_all(outgoing, "batch", split_axis=1, concat_axis=1, tiled=True)
    sender_table = lax.dynamic_slice(
        table_grid, (zero_index, my_half, zero_index), (batch_count, 1, slot_count)
    ).reshape(batch_count, slot_count)
    sequence_ids = sender_table // block_count
    arrivals = sequence_ids // SEQ_DEV == my_batch
    arrive_place = (
        jnp.arange(batch_count, dtype=jnp.int32)[:, None] * per_peer
        + jnp.cumsum(arrivals.astype(jnp.int32), axis=1)
        - 1
    )
    target = (
        (sequence_ids - my_batch * SEQ_DEV) * half_blocks
        + sender_table % block_count
        - my_half * half_blocks
    )
    target = jnp.where(arrivals, target, slot_count)
    source = (
        jnp.zeros((slot_count,), jnp.int32)
        .at[target.reshape(-1)]
        .set(arrive_place.reshape(-1), mode="drop")
    )
    serving = jnp.take(received, source, axis=1)
    half_length = half_blocks * BLK
    seq_count = query.shape[0]
    local_keys = serving[0].reshape(seq_count, half_length * width)
    score_scale = 1.0 / math.sqrt(HEAD_NOPE + ROPE)
    every_query = lax.all_gather(query, "heads", axis=2, tiled=True)
    all_heads = every_query.shape[2]
    row_count = QTOK * all_heads
    query_rows = every_query.reshape(seq_count, row_count, width)
    draft = jnp.arange(row_count, dtype=jnp.int32) // all_heads
    limits = lengths[:, None] - QTOK + draft[None, :]
    key_rows = local_keys.reshape(seq_count, half_length, width)
    highest, totals, mixed = partial_softmax(
        query_rows, key_rows, my_half * half_length, limits, score_scale
    )
    shaped = (
        highest.reshape(1, seq_count, QTOK, all_heads),
        totals.reshape(1, seq_count, QTOK, all_heads),
        mixed.reshape(1, seq_count, QTOK, all_heads, LATENT),
    )
    pieces = (
        lax.all_to_all(shaped[0], "heads", split_axis=3, concat_axis=0, tiled=True),
        lax.all_to_all(shaped[1], "heads", split_axis=3, concat_axis=0, tiled=True),
        lax.all_to_all(shaped[2], "heads", split_axis=3, concat_axis=0, tiled=True),
    )
    overall = jnp.max(pieces[0], axis=0)
    factor = jnp.exp(pieces[0] - overall[None])
    totals = jnp.sum(pieces[1] * factor, axis=0)
    mixed = jnp.sum(pieces[2] * factor[..., None], axis=0)
    context = (mixed / totals[..., None]).astype(jnp.bfloat16)
    return context


def send_orders(batch_count):
    whole = list(range(1, batch_count))
    if batch_count != 8:
        return [whole] * 8, [[0] + whole] * 8
    sends = [
        [1, 2, 3, 4, 5, 6, 7],
        [1, 2, 3, 4, 5, 6, 7],
        [7, 1, 2, 3, 6, 4, 5],
        [7, 1, 2, 3, 6, 4, 5],
        [7, 4, 5, 2, 3, 6, 1],
        [7, 4, 5, 2, 3, 6, 1],
        [6, 7, 2, 3, 1, 4, 5],
        [6, 7, 2, 3, 1, 4, 5],
    ]
    uses = [
        [0, 1, 6, 7, 4, 2, 5, 3],
        [0, 1, 6, 7, 4, 2, 5, 3],
        [0, 1, 2, 3, 7, 4, 6, 5],
        [0, 1, 2, 3, 7, 4, 6, 5],
        [0, 1, 7, 2, 4, 3, 6, 5],
        [0, 1, 7, 2, 4, 3, 6, 5],
        [0, 1, 2, 3, 6, 7, 4, 5],
        [0, 1, 2, 3, 6, 7, 4, 5],
    ]
    return sends, uses


def fused_kernel(
    batch_count, table_ref, length_ref, storage_ref, query_ref, out_ref,
    tabled, lengthy, stored, asked, outgoing, keys, queries, places, mixed,
    load_sem, fetch_sem, send_sem, recv_sem, pass_sem, take_sem, ready_sem, ahead_of,
):
    slot_count = stored.shape[0]
    per_peer = slot_count // batch_count
    block_count = MAXLEN // BLK
    width = LATENT + ROPE
    span = 2 * width
    pieces = BLK // 2
    me = lax.axis_index("batch")
    half = lax.axis_index("heads")
    sibling = 1 - half
    depth = me // 2
    deep = batch_count // 2
    left = depth == deep // 2 - 1
    right = depth == deep // 2
    middle = left | right
    across = batch_count - 1
    sends, uses = send_orders(batch_count)
    stage = jnp.where(left, 1, jnp.where(right, 2, jnp.where(depth < deep // 2, 0, 3)))
    kind = 2 * stage + me % 2

    def flip(step):
        other = me
        bit = 1
        while bit < batch_count:
            other = other + bit * (1 - 2 * ((me // bit) % 2)) * ((step // bit) % 2)
            bit *= 2
        return other

    def chosen(table, place):
        picked = table[0][place]
        for index in range(1, len(table)):
            if table[index][place] != table[0][place]:
                picked = jnp.where(kind == index, table[index][place], picked)
        return picked

    def columns(piece):
        return pl.ds(piece * span, span)

    def rows(index):
        return pl.ds(pl.multiple_of(index * per_peer, per_peer), per_peer)

    load_table = pltpu.make_async_copy(table_ref, tabled, load_sem.at[0])
    load_query = pltpu.make_async_copy(query_ref, asked, load_sem.at[1])
    load_length = pltpu.make_async_copy(length_ref, lengthy, load_sem.at[2])
    fetches = [
        pltpu.make_async_copy(
            storage_ref.at[:, columns(piece)], stored.at[:, columns(piece)], fetch_sem.at[piece]
        )
        for piece in range(pieces)
    ]
    load_table.start()
    for fetch in fetches:
        fetch.start()

    barrier = pltpu.get_barrier_semaphore()

    def tell(other, core):
        pl.semaphore_signal(
            barrier, inc=1, device_id={"batch": other, "heads": core}, device_id_type=MESH
        )

    @pl.when(middle)
    def _():
        tell(flip(across), half)

    for spot in range(batch_count):
        if spot // 2 in (deep // 2 - 1, deep // 2):
            continue
        for core in range(2):

            @pl.when((me != spot) | (half != core))
            def _():
                tell(spot, core)

    load_query.start()
    load_length.start()

    load_table.wait()
    table = tabled[...]
    row_ids = lax.broadcasted_iota(jnp.int32, table.shape, 0)
    square = (slot_count, slot_count)
    down = lax.broadcasted_iota(jnp.int32, square, 0)
    along = lax.broadcasted_iota(jnp.int32, square, 1)
    earlier = (down < along).astype(jnp.float32).astype(jnp.bfloat16)
    own = jnp.sum(jnp.where(row_ids == 2 * me + half, table, 0), axis=0, keepdims=True)
    owner = jnp.right_shift(own, block_count.bit_length() - 1)
    belongs = (row_ids == owner).astype(jnp.float32)
    counts = jnp.dot(belongs.astype(jnp.bfloat16), earlier, preferred_element_type=jnp.float32)
    rank = jnp.sum(belongs * counts, axis=0, keepdims=True).astype(jnp.int32)
    place = owner * per_peer + rank
    order = (down == place).astype(jnp.float32).astype(jnp.bfloat16)

    lanes = lax.broadcasted_iota(jnp.int32, (1, 2 * ROPE), 1)
    first_lanes = (lanes < ROPE).astype(jnp.float32).astype(jnp.bfloat16)
    last_lanes = (lanes >= ROPE).astype(jnp.float32).astype(jnp.bfloat16)

    def gather(picks, piece, target, base):
        moved = jnp.dot(picks, stored[:, columns(piece)], preferred_element_type=jnp.float32)
        target[:, base : base + LATENT] = moved[:, :LATENT].astype(jnp.bfloat16)
        target[:, base + LATENT : base + 2 * LATENT] = moved[
            :, width : width + LATENT
        ].astype(jnp.bfloat16)
        target[:, base + 2 * LATENT : base + span] = jnp.where(
            lanes < ROPE, moved[:, LATENT : LATENT + 2 * ROPE], moved[:, span - 2 * ROPE :]
        ).astype(jnp.bfloat16)

    def send(step, where):
        other = flip(step)
        return pltpu.make_async_remote_copy(
            src_ref=outgoing.at[rows(other), where],
            dst_ref=keys.at[half, rows(me), where],
            send_sem=send_sem,
            recv_sem=recv_sem.at[step - 1],
            device_id={"batch": other},
            device_id_type=MESH,
        )

    everything = pl.ds(0, pieces * span)

    def arrival(step):
        other = flip(step)
        return pltpu.make_async_remote_copy(
            src_ref=outgoing.at[rows(other), everything],
            dst_ref=keys.at[half, rows(other), everything],
            send_sem=send_sem,
            recv_sem=recv_sem.at[step - 1],
            device_id={"batch": other},
            device_id_type=MESH,
        )

    def hand_over(step, source):
        other = flip(step)
        return pltpu.make_async_remote_copy(
            src_ref=source.at[rows(other)],
            dst_ref=keys.at[half, rows(other)],
            send_sem=pass_sem,
            recv_sem=take_sem.at[step],
            device_id={"heads": sibling},
            device_id_type=MESH,
        )

    fetches[0].wait()

    @pl.when(middle)
    def _():
        beside = lax.broadcasted_iota(jnp.int32, (per_peer, slot_count), 0)
        picks = beside + flip(across) * per_peer == place
        gather(picks.astype(jnp.float32).astype(jnp.bfloat16), 0, ahead_of, 0)
        pl.semaphore_wait(barrier, 1)
        pltpu.make_async_remote_copy(
            src_ref=ahead_of,
            dst_ref=keys.at[half, rows(me), columns(0)],
            send_sem=send_sem,
            recv_sem=recv_sem.at[across - 1],
            device_id={"batch": flip(across)},
            device_id_type=MESH,
        ).start()

    for piece in list(range(1, pieces)) + [0]:
        if piece:
            fetches[piece].wait()
        gather(order, piece, outgoing, piece * span)
        if piece:

            @pl.when(middle)
            def _():
                send(across, columns(piece)).start()

    @pl.when(middle)
    def _():
        pl.semaphore_wait(ready_sem, 1)

    @pl.when(jnp.logical_not(middle))
    def _():
        pl.semaphore_wait(barrier, 2 * batch_count - 1)

        @pl.when((depth == 0) | (depth == deep - 1))
        def _():
            inner = jnp.where(depth == 0, me + batch_count - 2 - deep, me - batch_count + 2 + deep)
            pl.semaphore_signal(
                ready_sem, inc=1, device_id={"batch": inner}, device_id_type=MESH
            )

        send(chosen(sends, 0), everything).start()

    for turn in range(1, batch_count - 3):
        send(chosen(sends, turn), everything).start()

    held = depth == deep - 1

    def send_late(late):
        send(chosen(sends, batch_count - 3 + late), everything).start()

    @pl.when(jnp.logical_not(held))
    def _():
        for late in range(2):
            send_late(late)

    hand_over(0, outgoing).start()

    keys[half, rows(me)] = outgoing[rows(me)]

    mine = jnp.right_shift(table, block_count.bit_length() - 1) == me
    marks = mine.astype(jnp.float32)
    ranks = jnp.dot(
        marks.astype(jnp.bfloat16), earlier, preferred_element_type=jnp.float32
    ).astype(jnp.int32)
    ranks = jnp.where(mine, ranks, -1)
    blocks = jnp.bitwise_and(table, block_count - 1).astype(jnp.float32)
    lane = lax.broadcasted_iota(jnp.int32, table.shape, 1)
    spots = (lane // per_peer).astype(jnp.float32)
    for index in range(per_peer):
        number = jnp.sum(jnp.where(ranks == index, blocks, 0.0), axis=1, keepdims=True)
        spots = spots + jnp.where(lane % per_peer == index, number * BLK, 0.0)
    places[...] = spots

    row_count = asked.shape[0]
    heads = row_count // QTOK
    load_length.wait()
    limits = [(lengthy[0] - QTOK + draft).astype(jnp.float32) for draft in range(QTOK)]

    load_query.wait()
    asking = asked[...]
    queries[:, :width] = asking
    queries[:, width:] = asking[:, LATENT:]

    factor = math.log2(math.e) / math.sqrt(HEAD_NOPE + ROPE)
    portion = row_count // SHARES
    peaks = [jnp.full((portion, 1), -1e30, jnp.float32)] * SHARES
    totals = [None] * SHARES
    steps = [0] + [chosen(uses, turn) for turn in range(1, batch_count)]
    for turn in range(batch_count):
        if turn + AHEAD < batch_count:
            for ahead in range(1 if turn == 0 else turn + AHEAD, turn + AHEAD + 1):
                arrival(steps[ahead]).wait_recv()
                if ahead in HOLDS:

                    @pl.when(held)
                    def _():
                        send_late(HOLDS.index(ahead))

                hand_over(steps[ahead], keys.at[half]).start()
        step = steps[turn]
        other = me if turn == 0 else flip(step)
        hand_over(step, keys.at[half]).wait_recv()
        latents = []
        ropes = []
        for core in range(2):
            for piece in range(pieces):
                base = piece * span
                pair = keys[core, rows(other), base + 2 * LATENT : base + span]
                for parity in range(2):
                    low = base + parity * LATENT
                    latents.append(keys[core, rows(other), low : low + LATENT])
                    ropes.append(pair * (last_lanes if parity else first_lanes))
        latent = jnp.concatenate(latents, axis=0)
        rope = jnp.concatenate(ropes, axis=0)
        whole = jnp.concatenate([latent, rope], axis=1)
        at = places[pl.ds(2 * other, 2), :]
        at = jnp.concatenate([at[0:1], at[1:2]], axis=1)
        masks = [jnp.where(at <= limits[draft], 0.0, -1e30) for draft in range(QTOK)]
        for share in range(SHARES):
            low, high = share * portion, (share + 1) * portion
            dots = lax.dot_general(
                queries[low:high], whole, NT, preferred_element_type=jnp.float32
            )
            scores = jnp.concatenate(
                [
                    dots[draft * heads - low : (draft + 1) * heads - low] + masks[draft]
                    for draft in range(low // heads, high // heads)
                ],
                axis=0,
            )
            higher = jnp.maximum(peaks[share], jnp.max(scores, axis=1, keepdims=True))
            raised = jnp.exp2((scores - higher) * factor)
            sums = raised[:, :slot_count] + raised[:, slot_count:]
            fresh = jnp.dot(
                raised.astype(jnp.bfloat16), latent, preferred_element_type=jnp.float32
            )
            if turn == 0:
                totals[share] = sums
                mixed[low:high] = fresh
            else:
                shrink = jnp.exp2((peaks[share] - higher) * factor)
                totals[share] = totals[share] * shrink + sums
                mixed[low:high] = mixed[low:high] * shrink + fresh
            peaks[share] = higher
    for share in range(SHARES):
        low, high = share * portion, (share + 1) * portion
        inverse = 1.0 / jnp.sum(totals[share], axis=1, keepdims=True)
        out_ref[low:high] = (mixed[low:high] * inverse).astype(out_ref.dtype)
    others = pl.ds(0, slot_count - per_peer)
    pltpu.make_async_remote_copy(
        src_ref=outgoing.at[others],
        dst_ref=keys.at[half, others],
        send_sem=send_sem,
        recv_sem=recv_sem.at[0],
        device_id={"heads": sibling},
        device_id_type=MESH,
    ).wait_send()
    pltpu.make_async_remote_copy(
        src_ref=keys.at[half],
        dst_ref=keys.at[half],
        send_sem=pass_sem,
        recv_sem=take_sem.at[0],
        device_id={"heads": sibling},
        device_id_type=MESH,
    ).wait_send()


def local(storage, block_table, lengths, query):
    batch_count = lax.axis_size("batch")
    slot_count = storage.shape[1]
    per_peer = slot_count // batch_count
    whole = batch_count & (batch_count - 1) == 0 and query.shape[0] == SEQ_DEV
    whole = whole and batch_count >= 8 and lax.axis_size("heads") == 2
    if per_peer % 16 or slot_count != 128 or BLK * per_peer != slot_count or not whole:
        return plain_local(storage, block_table, lengths, query)
    width = LATENT + ROPE
    heads = query.shape[2]
    row_count = QTOK * heads
    vmem = pl.BlockSpec(memory_space=pltpu.VMEM)
    anywhere = pl.BlockSpec(memory_space=pltpu.HBM)
    context = pl.pallas_call(
        functools.partial(fused_kernel, batch_count),
        out_shape=jax.ShapeDtypeStruct((row_count, LATENT), jnp.bfloat16),
        in_specs=[anywhere] * 4,
        out_specs=vmem,
        scratch_shapes=[
            pltpu.VMEM((block_table.shape[0] // slot_count, slot_count), jnp.int32),
            pltpu.SMEM(lengths.shape, jnp.int32),
            pltpu.VMEM((slot_count, BLK * width), jnp.bfloat16),
            pltpu.VMEM((row_count, width), jnp.bfloat16),
            pltpu.VMEM((slot_count, BLK * width), jnp.bfloat16),
            pltpu.VMEM((2, slot_count, BLK * width), jnp.bfloat16),
            pltpu.VMEM((row_count, LATENT + 2 * ROPE), jnp.bfloat16),
            pltpu.VMEM((block_table.shape[0] // slot_count, slot_count), jnp.float32),
            pltpu.VMEM((row_count, LATENT), jnp.float32),
            pltpu.SemaphoreType.DMA((3,)),
            pltpu.SemaphoreType.DMA((BLK // 2,)),
            pltpu.SemaphoreType.DMA,
            pltpu.SemaphoreType.DMA((batch_count - 1,)),
            pltpu.SemaphoreType.DMA,
            pltpu.SemaphoreType.DMA((batch_count,)),
            pltpu.SemaphoreType.REGULAR,
            pltpu.VMEM((per_peer, 2 * width), jnp.bfloat16),
        ],
        compiler_params=pltpu.CompilerParams(collective_id=0, has_side_effects=True, vmem_limit_bytes=54800 * 1024),
    )(
        pltpu.with_memory_space_constraint(block_table.reshape(-1, slot_count), pltpu.HBM),
        lengths,
        storage[0],
        query.reshape(row_count, width),
    )
    return context.reshape(1, QTOK, heads, LATENT)


def solution(mesh):
    in_specs = (
        P(None, ("groups", "batch", "heads"), None),
        P("groups"),
        P(("groups", "batch")),
        P(("groups", "batch"), None, "heads", None),
    )
    out_specs = P(("groups", "batch"), None, "heads", None)
    return jax.shard_map(local, mesh=mesh, in_specs=in_specs, out_specs=out_specs, check_vma=False)
```
